256 devices in a mesh: batch: 8 (over x, core), cache: 32 (over y, z).
Axes of the slice: x: 4, y: 4, z: 8, core: 2. Of those that a mesh axis runs over, the one named last changes fastest.
Arguments:
- hidden_in: bfloat16 [64, 4096], P('batch'), may hold values from -6 to 6
- attn_gain: bfloat16 [4096], replicated, may hold values from 0.25 to 1.75
- w_query: bfloat16 [4096, 4096], P(None, 'cache'), may hold values from -0.09375 to 0.09375
- w_key: bfloat16 [4096, 1024], P(None, 'cache'), may hold values from -0.09375 to 0.09375
- w_value: bfloat16 [4096, 1024], P(None, 'cache'), may hold values from -0.09375 to 0.09375
- key_cache: bfloat16 [64, 4096, 1024], P('batch', 'cache'), may hold values from -400 to 400, as said below
- value_cache: bfloat16 [64, 4096, 1024], P('batch', 'cache'), may hold values from -6 to 6
- write_pos: int32 [64], P('batch'), may hold values from 0 to 12287, as said below
- cache_len: int32 [64], P('batch'), may hold values from 0 to 4095, as said below
- w_out: bfloat16 [4096, 4096], P('cache'), may hold values from -0.1875 to 0.1875
- mlp_gain: bfloat16 [4096], replicated, may hold values from 0.25 to 1.75
- w_gate: bfloat16 [4096, 7168], P(None, 'cache'), may hold values from -0.09375 to 0.09375
- w_up: bfloat16 [4096, 7168], P(None, 'cache'), may hold values from -0.09375 to 0.09375
- w_down: bfloat16 [7168, 4096], P('cache'), may hold values from -0.125 to 0.125
Outputs:
- hidden_out: bfloat16 [64, 4096], P('batch', 'cache')
The draws below stay inside these ranges and needn't reach their ends.
Inputs may be any that keep to these rules, and one draw needn't show every extreme that they name: `key_cache`: keys of earlier tokens are finite reals. `write_pos`: positions of the new tokens; the largest value occurs in every draw. cache_len never exceeds write_pos; both 0 and 4095 occur in every draw, and many sequences attend fewer than 4095 earlier tokens.
All inputs are finite; a program needn't handle non-finite values.
Results may differ from the reference program's by a relative error of at most 0.017.
Values may be sent and summed in bfloat16 or wider, within the bound.
A program may use at most 64 MiB of HBM per device.

```python
import jax
import jax.numpy as jnp
from jax import lax

D = 4096
HEADS = 32
KV_HEADS = 8
HEAD_DIM = 128
FFW = 7168
SEQS = 64
CACHE_SLOTS = 4096


def position_pair(key):
    inner = jax.random.fold_in(key, 11)
    first, second, third = jax.random.split(inner, 3)
    position = jax.random.randint(first, (SEQS,), 0, 3 * CACHE_SLOTS)
    position = position.at[0].set(3 * CACHE_SLOTS - 1)
    longest = jnp.minimum(position, CACHE_SLOTS - 1)
    partial_len = jax.random.randint(second, (SEQS,), 0, longest + 1)
    picked = jax.random.randint(third, (SEQS,), 0, 2)
    length = jnp.where(picked == 1, longest, partial_len)
    length = length.at[0].set(CACHE_SLOTS - 1)
    length = length.at[1].set(0)
    return (position.astype(jnp.int32), length.astype(jnp.int32))


def draw_write_pos(key, part):
    return position_pair(key)[0]


def draw_cache_len(key, part):
    return position_pair(key)[1]


def draw_key_cache(key, part):
    inner = jax.random.fold_in(key, 23)
    first = jax.random.fold_in(inner, 0)
    base = jnp.clip(jax.random.normal(first, (SEQS, CACHE_SLOTS, KV_HEADS * HEAD_DIM), jnp.float32), -6.0, 6.0)
    return base.astype(jnp.bfloat16)


def spiked(entries, rng, source, target, parts, factor):
    owner, partner = [(jnp.arange(entries.shape[dim]) // (entries.shape[dim] // parts)).reshape([-1 if axis == dim else 1 for axis in range(entries.ndim)]) for dim in (source, target)]
    chosen = jax.random.permutation(rng, parts)[partner]
    strong = (owner == chosen) | (owner == (partner + parts // 2) % parts)
    return jnp.where(strong, factor * entries, entries)


def block_levels(own_key, dims, pieces, least, top_value):
    level, own = 1.0, jax.random.fold_in(own_key, 6)
    for axis_at, parts in pieces:
        heights = jnp.exp(jax.random.uniform(jax.random.fold_in(own, axis_at), (parts,), jnp.float32, least / len(pieces), top_value / len(pieces)))
        level = level * jnp.repeat(heights, dims[axis_at] // parts).reshape([-1 if axis == axis_at else 1 for axis in range(len(dims))])
    return level


def normal_values(own_key, dims, deviation, most, cuts=(), kind=jnp.bfloat16):
    factor_of = block_levels(own_key, dims, cuts, -0.22, 0.18) if cuts else 1.0
    drawn = jax.random.normal(own_key, dims, jnp.float32) * deviation * factor_of
    return jnp.minimum(jnp.maximum(drawn, -most), most).astype(kind)


def heavy_noise(key, shape, scale, bound, shards, heavy, kind=jnp.bfloat16):
    values = scale * jax.random.normal(key, shape, jnp.float32)
    if shards:
        values = values * block_levels(key, shape, shards, -0.22, 0.18)
    return jnp.clip(spiked(values, jax.random.fold_in(key, 3), *heavy), -bound, bound).astype(kind)


def setup_inputs(seed: int = 0) -> dict:
    streams_of = jax.random.split(jax.random.key(seed), 15)
    hidden_in = normal_values(streams_of[0], (SEQS, D), 1.0, 6.0, ((0, 8),))
    attn_gain = jnp.clip(1.0 + 0.15 * jax.random.normal(streams_of[1], (D,), jnp.float32), 0.25, 1.75).astype(jnp.bfloat16)
    w_query = normal_values(streams_of[2], (D, HEADS * HEAD_DIM), D ** -0.5, 0.09375, ((1, 32),))
    w_key = normal_values(streams_of[3], (D, KV_HEADS * HEAD_DIM), D ** -0.5, 0.09375, ((1, 32),))
    w_value = normal_values(streams_of[4], (D, KV_HEADS * HEAD_DIM), D ** -0.5, 0.09375, ((1, 32),))
    key_cache = draw_key_cache(jax.random.fold_in(streams_of[14], 71), 0)
    value_cache = normal_values(streams_of[6], (SEQS, CACHE_SLOTS, KV_HEADS * HEAD_DIM), 1.0, 6.0, ((0, 8), (1, 32)))
    write_pos = draw_write_pos(jax.random.fold_in(streams_of[14], 71), 0)
    cache_len = draw_cache_len(jax.random.fold_in(streams_of[14], 71), 0)
    w_out = heavy_noise(streams_of[9], (HEADS * HEAD_DIM, D), (HEADS * HEAD_DIM) ** -0.5, 0.1875, ((0, 32),), (0, 1, 32, 2.75))
    mlp_gain = jnp.clip(1.0 + 0.15 * jax.random.normal(streams_of[10], (D,), jnp.float32), 0.25, 1.75).astype(jnp.bfloat16)
    w_gate = normal_values(streams_of[11], (D, FFW), D ** -0.5, 0.09375, ((1, 32),))
    w_up = normal_values(streams_of[12], (D, FFW), D ** -0.5, 0.09375, ((1, 32),))
    w_down = heavy_noise(streams_of[13], (FFW, D), FFW ** -0.5, 0.125, ((0, 32),), (0, 1, 32, 2.75))
    return dict(hidden_in=hidden_in, attn_gain=attn_gain, w_query=w_query, w_key=w_key, w_value=w_value, key_cache=key_cache, value_cache=value_cache, write_pos=write_pos, cache_len=cache_len, w_out=w_out, mlp_gain=mlp_gain, w_gate=w_gate, w_up=w_up, w_down=w_down)


def rms_norm(values, gain):
    wide = values.astype(jnp.float32)
    spread = lax.optimization_barrier(jnp.mean(wide * wide, axis=-1, keepdims=True))
    return (wide * lax.rsqrt(spread + 1e-05) * gain.astype(jnp.float32)).astype(jnp.bfloat16)

def rotate(heads, position):
    half = heads.shape[-1] // 2
    freq = 10000.0 ** (-(jnp.arange(half, dtype=jnp.float32) * 2.0 / heads.shape[-1]))
    angle = position.astype(jnp.float32)[:, None] * freq[None, :]
    cosine = jnp.cos(angle)[:, None, :]
    sine = jnp.sin(angle)[:, None, :]
    first = heads[..., :half]
    second = heads[..., half:]
    return jnp.concatenate([first * cosine - second * sine, second * cosine + first * sine], axis=-1)

def reference(hidden_in, attn_gain, w_query, w_key, w_value, key_cache, value_cache, write_pos, cache_len, w_out, mlp_gain, w_gate, w_up, w_down):
    seqs = hidden_in.shape[0]
    group = HEADS // KV_HEADS
    normed = rms_norm(hidden_in, attn_gain)
    query_raw = jnp.dot(normed, w_query, preferred_element_type=jnp.float32).astype(jnp.bfloat16)
    key_raw = jnp.dot(normed, w_key, preferred_element_type=jnp.float32).astype(jnp.bfloat16)
    value_new = jnp.dot(normed, w_value, preferred_element_type=jnp.float32).astype(jnp.bfloat16)
    query = rotate(query_raw.astype(jnp.float32).reshape(seqs, HEADS, HEAD_DIM), write_pos).astype(jnp.bfloat16)
    fresh_key_row = rotate(key_raw.astype(jnp.float32).reshape(seqs, KV_HEADS, HEAD_DIM), write_pos).astype(jnp.bfloat16)
    slots = jnp.arange(CACHE_SLOTS, dtype=jnp.int32)
    dist = (write_pos[:, None] - 1 - slots[None, :]) % CACHE_SLOTS + 1
    valid = dist <= cache_len[:, None]
    scale = 1.0 / HEAD_DIM ** 0.5

    def one_sequence(items):
        qrow, keys, values, knew, vnew, keep = items
        qwide = qrow.astype(jnp.float32).reshape(KV_HEADS, group, HEAD_DIM)
        kwide = keys.astype(jnp.float32).reshape(CACHE_SLOTS, KV_HEADS, HEAD_DIM)
        vwide = values.astype(jnp.float32).reshape(CACHE_SLOTS, KV_HEADS, HEAD_DIM)
        scores = jnp.einsum('kgd,wkd->kgw', qwide, kwide) * scale
        own = jnp.einsum('kgd,kd->kg', qwide, knew.astype(jnp.float32)) * scale
        scores = jnp.where(keep[None, None, :], scores, -1e+30)
        top = jnp.maximum(lax.optimization_barrier(jnp.max(scores, axis=-1)), own)
        weights = jnp.where(keep[None, None, :], jnp.exp(scores - top[..., None]), 0.0)
        own_weight = jnp.exp(own - top)
        total = lax.optimization_barrier(jnp.sum(weights, axis=-1)) + own_weight
        low = lax.optimization_barrier(weights.astype(jnp.bfloat16)).astype(jnp.float32)
        own_low = lax.optimization_barrier(own_weight.astype(jnp.bfloat16)).astype(jnp.float32)
        reduced_total = jnp.einsum('kgw,wkd->kgd', low, vwide) + own_low[..., None] * vnew.astype(jnp.float32)[:, None, :]
        return (reduced_total / total[..., None]).reshape(HEADS * HEAD_DIM).astype(jnp.bfloat16)
    attended = lax.map(one_sequence, (query, key_cache, value_cache, fresh_key_row, value_new.reshape(seqs, KV_HEADS, HEAD_DIM), valid))
    projected = jnp.dot(attended, w_out, preferred_element_type=jnp.float32)
    mid = (hidden_in.astype(jnp.float32) + projected).astype(jnp.bfloat16)
    normed_mid = rms_norm(mid, mlp_gain)
    gate = jnp.dot(normed_mid, w_gate, preferred_element_type=jnp.float32)
    upper = jnp.dot(normed_mid, w_up, preferred_element_type=jnp.float32)
    act = (jax.nn.silu(gate) * upper).astype(jnp.bfloat16)
    down = jnp.dot(act, w_down, preferred_element_type=jnp.float32)
    return (mid.astype(jnp.float32) + down).astype(jnp.bfloat16)
```

```python
import functools
import math

import jax
import jax.numpy as jnp
from jax import lax
from jax.experimental import pallas as pl
from jax.experimental.pallas import tpu as pltpu
from jax.sharding import PartitionSpec as P

HEADS = 32
KV_HEADS = 8
HEAD_DIM = 128
GROUP = HEADS // KV_HEADS
NY, NZ = 4, 8
N = NY * NZ
LOW = -1e30
MESH = pl.DeviceIdType.MESH
F32 = jnp.float32
BF16 = jnp.bfloat16

OFFSETS = sorted(
    [(dy, dz) for dy in range(NY) for dz in range(NZ) if (dy, dz) != (0, 0)],
    key=lambda t: -(min(t[0], NY - t[0]) + min(t[1], NZ - t[1])),
)


def row_sum(x):
    return jnp.sum(x, axis=-1, keepdims=True)


def dot_rows(a, b):
    return lax.dot_general(a, b, (((1,), (1,)), ((), ())), preferred_element_type=F32)


def split3(x):
    high = x.astype(BF16)
    rest = x - high.astype(F32)
    mid = rest.astype(BF16)
    low = (rest - mid.astype(F32)).astype(BF16)
    return high, mid, low


def kernel(
    hidden_hbm, gain_hbm, wq_hbm, wk_hbm, wv_hbm, kc_hbm, vc_hbm, pos_ref, len_ref,
    wo_hbm, mgain_hbm, wg_hbm, wu_hbm, wd_hbm,
    out_ref,
    hidden, gain, wq, wk, wv, kc, vc, wo, mgain, wg, wu, wd,
    qbuf, kvbuf, osend, orecv, psend, precv, midbuf, dsend, drecv,
    load_sem, send_sem, recv_sem, kv_send, kv_recv,
):
    me = lax.axis_index("cache")
    y, z = me // NZ, lax.rem(me, NZ)
    seqs = hidden.shape[0]
    width = hidden.shape[1]
    slots = kc.shape[1]

    peers = []
    for dy, dz in OFFSETS:
        peers.append((dy * NZ + dz, lax.rem(y + dy, NY) * NZ + lax.rem(z + dz, NZ)))

    def source(offset):
        dy, dz = offset // NZ, offset % NZ
        return lax.rem(y + NY - dy, NY) * NZ + lax.rem(z + NZ - dz, NZ)

    barrier = pltpu.get_barrier_semaphore()
    for _, peer in peers:
        pl.semaphore_signal(barrier, inc=1, device_id={"cache": peer}, device_id_type=MESH)

    pairs = [
        (hidden_hbm, hidden), (gain_hbm, gain), (wq_hbm, wq), (wk_hbm, wk), (wv_hbm, wv), (kc_hbm, kc),
        (vc_hbm, vc), (wo_hbm, wo), (mgain_hbm, mgain), (wg_hbm, wg), (wu_hbm, wu), (wd_hbm, wd),
    ]
    loads = [pltpu.make_async_copy(a, b, load_sem.at[i]) for i, (a, b) in enumerate(pairs)]
    for copy in loads:
        copy.start()
    l_hidden, l_gain, l_wq, l_wk, l_wv, l_kc, l_vc, l_wo, l_mgain, l_wg, l_wu, l_wd = loads

    def send_all(phase, piece, dst):
        copies = []
        for offset, peer in peers:
            copy = pltpu.make_async_remote_copy(
                src_ref=piece(peer), dst_ref=dst(offset), send_sem=send_sem.at[phase, offset],
                recv_sem=recv_sem.at[phase, offset], device_id={"cache": peer}, device_id_type=MESH,
            )
            copy.start()
            copies.append(copy)
        return copies

    lane = lax.broadcasted_iota(jnp.int32, (seqs, HEAD_DIM), 1)
    row = lax.broadcasted_iota(jnp.int32, (seqs, HEAD_DIM), 0)
    half = HEAD_DIM // 2
    pos = jnp.zeros((seqs, HEAD_DIM), jnp.int32)
    length = jnp.zeros((seqs, HEAD_DIM), jnp.int32)
    for s in range(seqs):
        pos = jnp.where(row == s, pos_ref[s], pos)
        length = jnp.where(row == s, len_ref[s], length)
    freq = jnp.exp(lax.rem(lane, half).astype(F32) * (-math.log(10000.0) / half))
    angle = pos.astype(F32) * freq
    cosine = jnp.cos(angle)
    sine = jnp.sin(angle) * jnp.where(lane < half, -1.0, 1.0)

    def rotate(x):
        return x * cosine + pltpu.roll(x, half, 1) * sine

    slot = me * slots + lane
    dist = jnp.bitwise_and(pos - 1 - slot, slots * N - 1) + 1
    valid = dist <= length

    l_hidden.wait()
    l_gain.wait()
    wide = hidden[...].astype(F32)
    scale = lax.rsqrt(row_sum(wide * wide) / width + 1e-5)
    chunks = []
    for c in range(width // 128):
        part = wide[:, c * 128 : (c + 1) * 128] * scale * gain[c : c + 1, :].astype(F32)
        chunks.append(part.astype(BF16))
    normed = jnp.concatenate(chunks, axis=1)
    l_wq.wait()
    query = jnp.dot(normed, wq[...], preferred_element_type=F32).astype(BF16).astype(F32)
    query = rotate(query).astype(BF16)
    qbuf[me] = query
    l_wk.wait()
    l_wv.wait()
    key_part = dot_rows(normed, wk[...]).astype(BF16)
    value_part = dot_rows(normed, wv[...]).astype(BF16)
    quarter = HEAD_DIM // GROUP
    place = lax.broadcasted_iota(jnp.int32, (quarter, HEAD_DIM), 1)
    origin = lax.broadcasted_iota(jnp.int32, (quarter, HEAD_DIM), 0)
    member = lax.rem(me, GROUP)
    spread = jnp.where(place == origin + member * quarter, 1.0, 0.0).astype(BF16)
    kvbuf[0, 0] = jnp.dot(key_part, spread, preferred_element_type=F32).astype(BF16)
    kvbuf[0, 1] = jnp.dot(value_part, spread, preferred_element_type=F32).astype(BF16)

    pl.semaphore_wait(barrier, N - 1)

    q_copies = send_all(0, lambda p: qbuf.at[me], lambda k: qbuf.at[me])
    kv_copies = []
    for k in range(1, GROUP):
        peer = me - member + lax.rem(member + k, GROUP)
        copy = pltpu.make_async_remote_copy(
            src_ref=kvbuf.at[0], dst_ref=kvbuf.at[k], send_sem=kv_send.at[k], recv_sem=kv_recv.at[k],
            device_id={"cache": peer}, device_id_type=MESH,
        )
        copy.start()
        kv_copies.append(copy)

    l_kc.wait()
    l_vc.wait()
    for copy in q_copies:
        copy.wait_recv()

    rows = GROUP * seqs
    row4 = lax.broadcasted_iota(jnp.int32, (rows, HEAD_DIM), 0)
    pick = [jnp.where(lax.rem(row4, seqs) == s, 1.0, 0.0).astype(BF16) for s in range(seqs)]
    valid4 = jnp.concatenate([valid] * GROUP, axis=0)
    lane4 = lax.rem(lax.broadcasted_iota(jnp.int32, (rows, HEAD_DIM), 1), 4)
    for g in range(KV_HEADS):
        cols = pl.ds(g * HEAD_DIM, HEAD_DIM)
        qg = qbuf[pl.ds(g * GROUP, GROUP)].reshape(rows, HEAD_DIM)
        left = jnp.concatenate([qg * pick[s] for s in range(seqs)], axis=1)
        keys = jnp.concatenate([kc[s, :, cols] for s in range(seqs)], axis=1)
        scores = dot_rows(left, keys)
        scores = jnp.where(valid4, scores * (1.0 / math.sqrt(HEAD_DIM)), LOW)
        top = jnp.max(scores, axis=-1, keepdims=True)
        weights = jnp.where(valid4, jnp.exp(scores - top), 0.0)
        total = row_sum(weights)
        low = weights.astype(BF16)
        left = jnp.concatenate([low * pick[s] for s in range(seqs)], axis=1)
        values = jnp.concatenate([vc[s, :, cols] for s in range(seqs)], axis=0)
        summed = jnp.dot(left, values, preferred_element_type=F32)
        some = total > 0.0
        safe = jnp.where(some, total, 1.0)
        share = (summed * (1.0 / safe)).astype(BF16)
        level = jnp.broadcast_to(jnp.where(some, top + jnp.log(safe), LOW), (rows, HEAD_DIM))
        high, mid, low3 = split3(level)
        stat = jnp.where(
            lane4 == 0, high.astype(F32), jnp.where(lane4 == 1, mid.astype(F32), jnp.where(lane4 == 2, low3.astype(F32), 0.0))
        ).astype(BF16)
        osend[pl.ds(g * GROUP, GROUP), 0] = share.reshape(GROUP, seqs, HEAD_DIM)
        osend[pl.ds(g * GROUP, GROUP), 1] = stat.reshape(GROUP, seqs, HEAD_DIM)

    o_copies = send_all(1, lambda p: osend.at[p], lambda k: orecv.at[k])

    for copy in kv_copies:
        copy.wait_recv()
    key_raw = kvbuf[0, 0].astype(F32)
    value_new = kvbuf[0, 1].astype(F32)
    for k in range(1, GROUP):
        key_raw = key_raw + kvbuf[k, 0].astype(F32)
        value_new = value_new + kvbuf[k, 1].astype(F32)
    key_new = rotate(key_raw).astype(BF16).astype(F32)
    own = row_sum(qbuf[me].astype(F32) * key_new) * (1.0 / math.sqrt(HEAD_DIM))
    own = jnp.broadcast_to(own, (seqs, HEAD_DIM))

    def level_of(stat):
        pair = stat + pltpu.roll(stat, 1, 1)
        return pair + pltpu.roll(pair, 2, 1)

    for copy in o_copies:
        copy.wait_recv()
    levels = [level_of(osend[me, 1].astype(F32))]
    for k in range(1, N):
        levels.append(level_of(orecv[k, 1].astype(F32)))
    peak = own
    for level in levels:
        peak = jnp.maximum(peak, level)
    factor = jnp.exp(own - peak)
    weight_sum = factor
    number = factor * value_new
    for k in range(N):
        share = (osend[me, 0] if k == 0 else orecv[k, 0]).astype(F32)
        factor = jnp.exp(levels[k] - peak)
        weight_sum = weight_sum + factor
        number = number + factor * share
    attended = (number / weight_sum).astype(BF16)

    def scatter(phase, left, weight, stage, landing):
        for c in range(N):
            part = jnp.dot(left, weight[:, c * 128 : (c + 1) * 128], preferred_element_type=F32)
            stage[c] = part.astype(BF16)
        return send_all(phase, lambda p: stage.at[p], lambda k: landing.at[k])

    def gathered(copies, stage, landing):
        for copy in copies:
            copy.wait_recv()
        total = stage[me].astype(F32)
        for k in range(1, N):
            total = total + landing[k].astype(F32)
        return total

    l_wo.wait()
    p_copies = scatter(2, attended, wo, psend, precv)
    mine = pl.ds(pl.multiple_of(me * 128, 128), 128)
    mid_own = (hidden[:, mine].astype(F32) + gathered(p_copies, psend, precv)).astype(BF16)
    midbuf[me] = mid_own
    m_copies = send_all(3, lambda p: midbuf.at[me], lambda k: midbuf.at[me])
    l_mgain.wait()
    l_wg.wait()
    l_wu.wait()
    l_wd.wait()
    for copy in m_copies:
        copy.wait_recv()
    squares = jnp.zeros((seqs, 128), F32)
    for c in range(N):
        part = midbuf[c].astype(F32)
        squares = squares + part * part
    scale = lax.rsqrt(row_sum(squares) / width + 1e-5)
    chunks = []
    for c in range(N):
        chunks.append((midbuf[c].astype(F32) * scale * mgain[c : c + 1, :].astype(F32)).astype(BF16))
    normed_mid = jnp.concatenate(chunks, axis=1)
    gate = dot_rows(normed_mid, wg[...])
    upper = dot_rows(normed_mid, wu[...])
    act = (gate / (1.0 + jnp.exp(-gate)) * upper).astype(BF16)
    d_copies = scatter(4, act, wd, dsend, drecv)
    total = gathered(d_copies, dsend, drecv)
    out_ref[...] = (mid_own.astype(F32) + total).astype(BF16)

    for copy in q_copies + kv_copies + o_copies + p_copies + m_copies + d_copies:
        copy.wait_send()


def per_device(*args):
    (hidden_in, attn_gain, w_query, w_key, w_value, key_cache, value_cache, write_pos, cache_len, w_out, mlp_gain,
     w_gate, w_up, w_down) = args
    seqs, width = hidden_in.shape
    lines = width // 128
    attn_gain = attn_gain.reshape(lines, 128)
    mlp_gain = mlp_gain.reshape(lines, 128)
    w_key, w_value, w_gate, w_up = w_key.T, w_value.T, w_gate.T, w_up.T
    any_space = pl.BlockSpec(memory_space=pl.ANY)
    smem = pl.BlockSpec(memory_space=pltpu.SMEM)
    operands = (hidden_in, attn_gain, w_query, w_key, w_value, key_cache, value_cache, write_pos, cache_len, w_out,
                mlp_gain, w_gate, w_up, w_down)
    loaded = [a for a in operands if a is not write_pos and a is not cache_len]
    block = (N, seqs, 128)
    return pl.pallas_call(
        kernel,
        out_shape=jax.ShapeDtypeStruct((seqs, 128), BF16),
        in_specs=[any_space] * 7 + [smem] * 2 + [any_space] * 5,
        out_specs=pl.BlockSpec(memory_space=pltpu.VMEM),
        scratch_shapes=[pltpu.VMEM(a.shape, a.dtype) for a in loaded]
        + [
            pltpu.VMEM(block, BF16),
            pltpu.VMEM((GROUP, 2, seqs, 128), BF16),
            pltpu.VMEM((N, 2, seqs, 128), BF16),
            pltpu.VMEM((N, 2, seqs, 128), BF16),
            pltpu.VMEM(block, BF16),
            pltpu.VMEM(block, BF16),
            pltpu.VMEM(block, BF16),
            pltpu.VMEM(block, BF16),
            pltpu.VMEM(block, BF16),
            pltpu.SemaphoreType.DMA((len(loaded),)),
            pltpu.SemaphoreType.DMA((5, N)),
            pltpu.SemaphoreType.DMA((5, N)),
            pltpu.SemaphoreType.DMA((GROUP,)),
            pltpu.SemaphoreType.DMA((GROUP,)),
        ],
        compiler_params=pltpu.CompilerParams(
            collective_id=0, has_side_effects=True, vmem_limit_bytes=60 * 1024 * 1024
        ),
    )(*operands)


def solution(mesh):
    in_specs = (
        P("batch", None),
        P(),
        P(None, "cache"),
        P(None, "cache"),
        P(None, "cache"),
        P("batch", "cache", None),
        P("batch", "cache", None),
        P("batch"),
        P("batch"),
        P("cache", None),
        P(),
        P(None, "cache"),
        P(None, "cache"),
        P("cache", None),
    )
    return jax.shard_map(
        per_device, mesh=mesh, in_specs=in_specs, out_specs=P("batch", "cache"), check_vma=False
    )
```

```python
import functools
import math

import jax
import jax.numpy as jnp
from jax import lax
from jax.experimental import pallas as pl
from jax.experimental.pallas import tpu as pltpu
from jax.sharding import PartitionSpec as P

HEADS = 32
KV_HEADS = 8
HEAD_DIM = 128
GROUP = HEADS // KV_HEADS
NY, NZ = 4, 8
N = NY * NZ
LOW = -1e30
MESH = pl.DeviceIdType.MESH
F32 = jnp.float32
BF16 = jnp.bfloat16

OFFSETS = sorted(
    [(dy, dz) for dy in range(NY) for dz in range(NZ) if (dy, dz) != (0, 0)],
    key=lambda t: -(min(t[0], NY - t[0]) + min(t[1], NZ - t[1])),
)
DISTANCE = [min(dy, NY - dy) + min(dz, NZ - dz) for dy, dz in OFFSETS]
BATCHES = (((0, 0), (0, 1), (1, 0), (3, 0)), ((1, 1), (3, 1), (2, 0)), ((2, 1),))


def row_sum(x):
    return jnp.sum(x, axis=-1, keepdims=True)


def dot_rows(a, b):
    return lax.dot_general(a, b, (((1,), (1,)), ((), ())), preferred_element_type=F32)


def split3(x):
    high = x.astype(BF16)
    rest = x - high.astype(F32)
    mid = rest.astype(BF16)
    low = (rest - mid.astype(F32)).astype(BF16)
    return high, mid, low


def kernel(
    hidden_hbm, gain_hbm, wq_hbm, wk_hbm, wv_hbm, kc_hbm, vc_hbm, pos_hbm, len_hbm,
    wo_hbm, mgain_hbm, wg_hbm, wu_hbm, wd_hbm,
    out_ref,
    hidden, gain, wq, wk, wv, kc, vc, pos_ref, len_ref, wo, mgain, wg, wu, wd,
    qbuf, kvbuf, osend, orecv, psend, precv, midbuf, dsend, drecv, mgain_wide,
    load_sem, send_sem, recv_sem, kv_send, kv_recv,
):
    me = lax.axis_index("cache")
    y, z = me // NZ, lax.rem(me, NZ)
    seqs = hidden.shape[0]
    width = hidden.shape[1]
    slots = kc.shape[1]

    peers = [lax.rem(y + dy, NY) * NZ + lax.rem(z + dz, NZ) for dy, dz in OFFSETS]

    barrier = pltpu.get_barrier_semaphore()
    for peer in peers:
        pl.semaphore_signal(barrier, inc=1, device_id={"cache": peer}, device_id_type=MESH)

    pairs = [
        (hidden_hbm, hidden), (gain_hbm, gain), (pos_hbm, pos_ref), (len_hbm, len_ref), (wq_hbm, wq), (wk_hbm, wk),
        (wv_hbm, wv), (kc_hbm, kc), (vc_hbm, vc), (wo_hbm, wo), (mgain_hbm, mgain), (wg_hbm, wg), (wu_hbm, wu),
        (wd_hbm, wd),
    ]
    loads = [pltpu.make_async_copy(a, b, load_sem.at[i]) for i, (a, b) in enumerate(pairs)]
    for copy in loads:
        copy.start()
    l_hidden, l_gain, l_pos, l_len, l_wq, l_wk, l_wv, l_kc, l_vc, l_wo, l_mgain, l_wg, l_wu, l_wd = loads

    def send(phase, src, dst, peer):
        copy = pltpu.make_async_remote_copy(
            src_ref=src, dst_ref=dst, send_sem=send_sem.at[phase, peer], recv_sem=recv_sem.at[phase, me],
            device_id={"cache": peer}, device_id_type=MESH,
        )
        copy.start()
        return copy

    def arrived(phase, ref, peer):
        pltpu.make_async_remote_copy(
            src_ref=ref, dst_ref=ref, send_sem=send_sem.at[phase, peer], recv_sem=recv_sem.at[phase, peer],
            device_id={"cache": peer}, device_id_type=MESH,
        ).wait_recv()

    def sent(copies):
        for copy in copies:
            copy.wait_send()

    lane = lax.broadcasted_iota(jnp.int32, (seqs, HEAD_DIM), 1)
    row = lax.broadcasted_iota(jnp.int32, (seqs, HEAD_DIM), 0)
    half = HEAD_DIM // 2
    l_pos.wait()
    l_len.wait()
    pos = jnp.zeros((seqs, HEAD_DIM), jnp.int32)
    length = jnp.zeros((seqs, HEAD_DIM), jnp.int32)
    for s in range(seqs):
        pos = jnp.where(row == s, pos_ref[s], pos)
        length = jnp.where(row == s, len_ref[s], length)
    freq = jnp.exp(lax.rem(lane, half).astype(F32) * (-math.log(10000.0) / half))
    angle = pos.astype(F32) * freq
    cosine = jnp.cos(angle)
    sine = jnp.sin(angle) * jnp.where(lane < half, -1.0, 1.0)

    def rotate(x):
        return x * cosine + pltpu.roll(x, half, 1) * sine

    slot = me * slots + lane
    dist = jnp.bitwise_and(pos - 1 - slot, slots * N - 1) + 1
    valid = dist <= length

    l_hidden.wait()
    l_gain.wait()
    wide = hidden[...].astype(F32)
    scale = lax.rsqrt(row_sum(wide * wide) / width + 1e-5)
    chunks = []
    for c in range(width // 128):
        part = wide[:, c * 128 : (c + 1) * 128] * scale * gain[c : c + 1, :].astype(F32)
        chunks.append(part.astype(BF16))
    normed = jnp.concatenate(chunks, axis=1)
    l_wq.wait()
    query = jnp.dot(normed, wq[...], preferred_element_type=F32).astype(BF16).astype(F32)
    query = rotate(query).astype(BF16)
    qbuf[me] = query

    pl.semaphore_wait(barrier, N - 1)
    q_copies = [send(0, qbuf.at[me], qbuf.at[me], peer) for peer in peers]

    l_wk.wait()
    l_wv.wait()
    key_part = dot_rows(normed, wk[...]).astype(BF16)
    value_part = dot_rows(normed, wv[...]).astype(BF16)
    quarter = HEAD_DIM // GROUP
    place = lax.broadcasted_iota(jnp.int32, (quarter, HEAD_DIM), 1)
    origin = lax.broadcasted_iota(jnp.int32, (quarter, HEAD_DIM), 0)
    member = lax.rem(me, GROUP)
    spread = jnp.where(place == origin + member * quarter, 1.0, 0.0).astype(BF16)
    kvbuf[0, 0] = jnp.dot(key_part, spread, preferred_element_type=F32).astype(BF16)
    kvbuf[0, 1] = jnp.dot(value_part, spread, preferred_element_type=F32).astype(BF16)
    mates = [me - member + lax.rem(member + k, GROUP) for k in range(1, GROUP)]
    kv_copies = []
    for k, peer in enumerate(mates, 1):
        copy = pltpu.make_async_remote_copy(
            src_ref=kvbuf.at[0], dst_ref=kvbuf.at[k], send_sem=kv_send.at[k], recv_sem=kv_recv.at[k],
            device_id={"cache": peer}, device_id_type=MESH,
        )
        copy.start()
        kv_copies.append(copy)

    rows = GROUP * seqs
    row4 = lax.broadcasted_iota(jnp.int32, (rows, HEAD_DIM), 0)
    pick = [jnp.where(lax.rem(row4, seqs) == s, 1.0, 0.0).astype(BF16) for s in range(seqs)]
    valid4 = jnp.concatenate([valid] * GROUP, axis=0)
    lane4 = lax.rem(lax.broadcasted_iota(jnp.int32, (rows, HEAD_DIM), 1), 4)

    def attend(g):
        cols = pl.ds(pl.multiple_of(g * HEAD_DIM, HEAD_DIM), HEAD_DIM)
        qg = qbuf[pl.ds(g * GROUP, GROUP)].reshape(rows, HEAD_DIM)
        left = jnp.concatenate([qg * pick[s] for s in range(seqs)], axis=1)
        keys = jnp.concatenate([kc[s, :, cols] for s in range(seqs)], axis=1)
        scores = dot_rows(left, keys)
        scores = jnp.where(valid4, scores * (1.0 / math.sqrt(HEAD_DIM)), LOW)
        top = jnp.max(scores, axis=-1, keepdims=True)
        weights = jnp.where(valid4, jnp.exp(scores - top), 0.0)
        total = row_sum(weights)
        low = weights.astype(BF16)
        left = jnp.concatenate([low * pick[s] for s in range(seqs)], axis=1)
        values = jnp.concatenate([vc[s, :, cols] for s in range(seqs)], axis=0)
        summed = jnp.dot(left, values, preferred_element_type=F32)
        some = total > 0.0
        safe = jnp.where(some, total, 1.0)
        share = (summed * (1.0 / safe)).astype(BF16)
        level = jnp.broadcast_to(jnp.where(some, top + jnp.log(safe), LOW), (rows, HEAD_DIM))
        high, mid, low3 = split3(level)
        stat = jnp.where(
            lane4 == 0, high.astype(F32),
            jnp.where(lane4 == 1, mid.astype(F32), jnp.where(lane4 == 2, low3.astype(F32), 0.0)),
        ).astype(BF16)
        osend[pl.ds(g * GROUP, GROUP), 0] = share.reshape(GROUP, seqs, HEAD_DIM)
        osend[pl.ds(g * GROUP, GROUP), 1] = stat.reshape(GROUP, seqs, HEAD_DIM)

    side = z // GROUP

    def group_at(dy, ds):
        return lax.rem(y + dy, NY) * 2 + lax.rem(side + ds, 2)

    def members(dy, ds):
        if (dy, ds) == (0, 0):
            return mates
        return [group_at(dy, ds) * GROUP + j for j in range(GROUP)]

    l_kc.wait()
    l_vc.wait()
    o_copies = []
    for batch in BATCHES:
        for dy, ds in batch:
            for peer in members(dy, ds):
                arrived(0, qbuf.at[peer], peer)
        for dy, ds in batch:
            attend(group_at(dy, ds))
        for dy, ds in reversed(batch):
            for peer in members(dy, ds):
                o_copies.append(send(1, osend.at[peer], orecv.at[me], peer))
    sent(q_copies)

    for copy in kv_copies:
        copy.wait_recv()
    key_raw = kvbuf[0, 0].astype(F32)
    value_new = kvbuf[0, 1].astype(F32)
    for k in range(1, GROUP):
        key_raw = key_raw + kvbuf[k, 0].astype(F32)
        value_new = value_new + kvbuf[k, 1].astype(F32)
    key_new = rotate(key_raw).astype(BF16).astype(F32)
    own = row_sum(qbuf[me].astype(F32) * key_new) * (1.0 / math.sqrt(HEAD_DIM))
    own = jnp.broadcast_to(own, (seqs, HEAD_DIM))
    sent(kv_copies)
    l_wo.wait()
    l_mgain.wait()
    l_wg.wait()
    l_wu.wait()
    l_wd.wait()
    mgain_wide[...] = mgain[...].astype(F32)

    def level_of(stat):
        pair = stat + pltpu.roll(stat, 1, 1)
        return pair + pltpu.roll(pair, 2, 1)

    def merge(state, parts):
        peak, weight_sum, number = state
        levels = [level_of(ref[1].astype(F32)) for ref in parts]
        top = peak
        for level in levels:
            top = jnp.maximum(top, level)
        factor = jnp.exp(peak - top)
        weight_sum = weight_sum * factor
        number = number * factor
        for level, ref in zip(levels, parts):
            factor = jnp.exp(level - top)
            weight_sum = weight_sum + factor
            number = number + factor * ref[0].astype(F32)
        return top, weight_sum, number

    state = merge((own, jnp.ones((seqs, HEAD_DIM), F32), value_new), [osend.at[me]])
    for least, most in ((0, 3), (4, 4), (5, 6)):
        near = [p for p, d in zip(peers, DISTANCE) if least <= d <= most]
        for peer in near:
            arrived(1, orecv.at[peer], peer)
        state = merge(state, [orecv.at[peer] for peer in near])
    attended = (state[2] / state[1]).astype(BF16)

    def scatter(phase, left, weight, stage, landing):
        copies = []
        order = peers + [me]
        for first in range(0, N, 8):
            part_of = order[first : first + 8]
            for p in part_of:
                cols = pl.ds(pl.multiple_of(p * 128, 128), 128)
                stage[p] = jnp.dot(left, weight[:, cols], preferred_element_type=F32).astype(BF16)
            for p in part_of:
                if p is not me:
                    copies.append(send(phase, stage.at[p], landing.at[me], p))
        return copies

    def gathered(phase, stage, landing):
        total = stage[me].astype(F32)
        for peer in reversed(peers):
            arrived(phase, landing.at[peer], peer)
            total = total + landing[peer].astype(F32)
        return total

    p_copies = scatter(2, attended, wo, psend, precv)
    sent(o_copies)
    mine = pl.ds(pl.multiple_of(me * 128, 128), 128)
    mid_own = (hidden[:, mine].astype(F32) + gathered(2, psend, precv)).astype(BF16)
    midbuf[me] = mid_own
    m_copies = [send(3, midbuf.at[me], midbuf.at[me], peer) for peer in peers]
    sent(p_copies)

    squares = jnp.zeros((seqs, 128), F32)
    gate = jnp.zeros((seqs, wg.shape[0]), F32)
    upper = jnp.zeros((seqs, wg.shape[0]), F32)
    for least, most in ((0, 2), (3, 3), (4, 4), (5, 6)):
        near = [p for p, d in zip(peers, DISTANCE) if least <= d <= most]
        for peer in near:
            arrived(3, midbuf.at[peer], peer)
        if least == 0:
            near = near + [me]
        parts = []
        for peer in near:
            part = midbuf[peer].astype(F32)
            squares = squares + part * part
            parts.append((part * mgain_wide[pl.ds(peer, 1), :]).astype(BF16))
        left = jnp.concatenate(parts, axis=1)
        places = [pl.ds(pl.multiple_of(p * 128, 128), 128) for p in near]
        gate = gate + dot_rows(left, jnp.concatenate([wg[:, c] for c in places], axis=1))
        upper = upper + dot_rows(left, jnp.concatenate([wu[:, c] for c in places], axis=1))
    scale = lax.rsqrt(row_sum(squares) / width + 1e-5)
    gate = gate * scale
    act = (gate / (1.0 + jnp.exp(-gate)) * (upper * scale)).astype(BF16)
    d_copies = scatter(4, act, wd, dsend, drecv)
    sent(m_copies)
    total = gathered(4, dsend, drecv)
    out_ref[...] = (mid_own.astype(F32) + total).astype(BF16)
    sent(d_copies)


def per_device(*args):
    (hidden_in, attn_gain, w_query, w_key, w_value, key_cache, value_cache, write_pos, cache_len, w_out, mlp_gain,
     w_gate, w_up, w_down) = args
    seqs, width = hidden_in.shape
    lines = width // 128
    attn_gain = attn_gain.reshape(lines, 128)
    mlp_gain = mlp_gain.reshape(lines, 128)
    w_key, w_value, w_gate, w_up = w_key.T, w_value.T, w_gate.T, w_up.T
    operands = (hidden_in, attn_gain, w_query, w_key, w_value, key_cache, value_cache, write_pos, cache_len, w_out,
                mlp_gain, w_gate, w_up, w_down)
    held = [pltpu.VMEM(a.shape, a.dtype) for a in operands]
    held[7] = pltpu.SMEM(write_pos.shape, write_pos.dtype)
    held[8] = pltpu.SMEM(cache_len.shape, cache_len.dtype)
    block = (N, seqs, 128)
    return pl.pallas_call(
        kernel,
        out_shape=jax.ShapeDtypeStruct((seqs, 128), BF16),
        in_specs=[pl.BlockSpec(memory_space=pltpu.HBM)] * len(operands),
        out_specs=pl.BlockSpec(memory_space=pltpu.VMEM),
        scratch_shapes=held
        + [
            pltpu.VMEM(block, BF16),
            pltpu.VMEM((GROUP, 2, seqs, 128), BF16),
            pltpu.VMEM((N, 2, seqs, 128), BF16),
            pltpu.VMEM((N, 2, seqs, 128), BF16),
            pltpu.VMEM(block, BF16),
            pltpu.VMEM(block, BF16),
            pltpu.VMEM(block, BF16),
            pltpu.VMEM(block, BF16),
            pltpu.VMEM(block, BF16),
            pltpu.VMEM((lines, 128), F32),
            pltpu.SemaphoreType.DMA((len(operands),)),
            pltpu.SemaphoreType.DMA((5, N)),
            pltpu.SemaphoreType.DMA((5, N)),
            pltpu.SemaphoreType.DMA((GROUP,)),
            pltpu.SemaphoreType.DMA((GROUP,)),
        ],
        compiler_params=pltpu.CompilerParams(
            collective_id=0, has_side_effects=True, vmem_limit_bytes=67043328
        ),
    )(*operands)


def solution(mesh):
    in_specs = (
        P("batch", None),
        P(),
        P(None, "cache"),
        P(None, "cache"),
        P(None, "cache"),
        P("batch", "cache", None),
        P("batch", "cache", None),
        P("batch"),
        P("batch"),
        P("cache", None),
        P(),
        P(None, "cache"),
        P(None, "cache"),
        P("cache", None),
    )
    return jax.shard_map(
        per_device, mesh=mesh, in_specs=in_specs, out_specs=P("batch", "cache"), check_vma=False
    )
```

```python
import functools
import math

import jax
import jax.numpy as jnp
from jax import lax
from jax.experimental import pallas as pl
from jax.experimental.pallas import tpu as pltpu
from jax.sharding import PartitionSpec as P

HEADS = 32
KV_HEADS = 8
HEAD_DIM = 128
GROUP = HEADS // KV_HEADS
NY, NZ = 4, 8
N = NY * NZ
LOW = -1e30
MESH = pl.DeviceIdType.MESH
F32 = jnp.float32
BF16 = jnp.bfloat16

OFFSETS = sorted(
    [(dy, dz) for dy in range(NY) for dz in range(NZ) if (dy, dz) != (0, 0)],
    key=lambda t: -(min(t[0], NY - t[0]) + min(t[1], NZ - t[1])),
)
DISTANCE = [min(dy, NY - dy) + min(dz, NZ - dz) for dy, dz in OFFSETS]
MID_CLASSES = ((1, 2), (3, 3), (4, 4), (5, 6))
NEAR = 4
BATCHES = (((0, 0), (0, 1), (1, 0), (3, 0)), ((1, 1), (3, 1), (2, 0)), ((2, 1),))


def mid_class(distance):
    return [least <= distance <= most for least, most in MID_CLASSES].index(True)


def row_sum(x):
    return jnp.sum(x, axis=-1, keepdims=True)


def dot_rows(a, b):
    return lax.dot_general(a, b, (((1,), (1,)), ((), ())), preferred_element_type=F32)


def split3(x):
    high = x.astype(BF16)
    rest = x - high.astype(F32)
    mid = rest.astype(BF16)
    low = (rest - mid.astype(F32)).astype(BF16)
    return high, mid, low


def kernel(
    hidden_hbm, gain_hbm, wq_hbm, wk_hbm, wv_hbm, kc_hbm, vc_hbm, pos_hbm, len_hbm,
    wo_hbm, mgain_hbm, wg_hbm, wu_hbm, wd_hbm,
    out_ref,
    hidden, gain, wq, wk, wv, kc, vc, pos_ref, len_ref, wo, mgain, wg, wu, wd,
    qbuf, kvbuf, osend, orecv, psend, precv, midbuf, dsend, drecv, mgain_wide,
    load_sem, send_sem, q_sem, kv_sem, o_sem, p_sem, m_sem, d_sem,
):
    me = lax.axis_index("cache")
    y, z = lax.shift_right_logical(me, 3), jnp.bitwise_and(me, NZ - 1)
    seqs = hidden.shape[0]
    width = hidden.shape[1]
    slots = kc.shape[2]

    rows_at = [jnp.bitwise_and(y + dy, NY - 1) * NZ for dy in range(NY)]
    cols_at = [jnp.bitwise_and(z + dz, NZ - 1) for dz in range(NZ)]
    peers = [rows_at[dy] + cols_at[dz] for dy, dz in OFFSETS]

    def at_distance(least, most):
        return [p for p, d in zip(peers, DISTANCE) if least <= d <= most]

    barrier = pltpu.get_barrier_semaphore()
    for peer in peers:
        pl.semaphore_signal(barrier, inc=1, device_id={"cache": peer}, device_id_type=MESH)

    def block(c):
        return pl.ds(pl.multiple_of(c * 128, 128), 128)

    plain = [
        (hidden_hbm, hidden), (gain_hbm, gain), (pos_hbm, pos_ref), (len_hbm, len_ref), (wq_hbm, wq), (wk_hbm, wk),
        (wv_hbm, wv), (mgain_hbm, mgain),
    ]
    loads = [pltpu.make_async_copy(a, b, load_sem.at[i]) for i, (a, b) in enumerate(plain)]
    for copy in loads:
        copy.start()
    l_hidden, l_gain, l_pos, l_len, l_wq, l_wk, l_wv, l_mgain = loads
    first = len(plain)
    for g in range(KV_HEADS):
        pltpu.make_async_copy(kc_hbm.at[:, :, block(g)], kc.at[g], load_sem.at[first]).start()
    for g in range(KV_HEADS):
        pltpu.make_async_copy(vc_hbm.at[:, :, block(g)], vc.at[g], load_sem.at[first + 1]).start()
    weights = ((wo_hbm, wo), (wg_hbm, wg), (wu_hbm, wu), (wd_hbm, wd))

    def load_weights(c, _):
        for i, (a, b) in enumerate(weights):
            pltpu.make_async_copy(a.at[:, block(c)], b.at[c], load_sem.at[first + 2 + i]).start()
        return 0

    def loaded(i, ref):
        pltpu.make_async_copy(ref, ref, load_sem.at[first + i]).wait()

    def send(phase, src, dst, recv_sem, peer):
        pltpu.make_async_remote_copy(
            src_ref=src, dst_ref=dst, send_sem=send_sem.at[phase], recv_sem=recv_sem,
            device_id={"cache": peer}, device_id_type=MESH,
        ).start()

    def pending(phase, ref, recv_sem):
        return pltpu.make_async_remote_copy(
            src_ref=ref, dst_ref=ref, send_sem=send_sem.at[phase], recv_sem=recv_sem,
            device_id={"cache": peers[0]}, device_id_type=MESH,
        )

    def arrived(recv_sem, ref):
        pending(0, ref, recv_sem).wait_recv()

    def sent(phase, ref):
        pending(phase, ref, kv_sem.at[0]).wait_send()

    def some(buffer, count):
        return buffer.at[pl.ds(0, count)]

    lane = lax.broadcasted_iota(jnp.int32, (seqs, HEAD_DIM), 1)
    row = lax.broadcasted_iota(jnp.int32, (seqs, HEAD_DIM), 0)
    half = HEAD_DIM // 2
    l_pos.wait()
    l_len.wait()
    pos = jnp.zeros((seqs, HEAD_DIM), jnp.int32)
    length = jnp.zeros((seqs, HEAD_DIM), jnp.int32)
    for s in range(seqs):
        pos = jnp.where(row == s, pos_ref[s], pos)
        length = jnp.where(row == s, len_ref[s], length)
    freq = jnp.exp(lax.rem(lane, half).astype(F32) * (-math.log(10000.0) / half))
    angle = pos.astype(F32) * freq
    cosine = jnp.cos(angle)
    sine = jnp.sin(angle) * jnp.where(lane < half, -1.0, 1.0)

    def rotate(x):
        return x * cosine + pltpu.roll(x, half, 1) * sine

    slot = me * slots + lane
    dist = jnp.bitwise_and(pos - 1 - slot, slots * N - 1) + 1
    valid = dist <= length

    l_hidden.wait()
    l_gain.wait()
    wide = hidden[...].astype(F32)
    scale = lax.rsqrt(row_sum(wide * wide) / width + 1e-5)
    chunks = []
    for c in range(width // 128):
        part = wide[:, c * 128 : (c + 1) * 128] * scale * gain[c : c + 1, :].astype(F32)
        chunks.append(part.astype(BF16))
    normed = jnp.concatenate(chunks, axis=1)
    l_wq.wait()
    query = jnp.dot(normed, wq[...], preferred_element_type=F32).astype(BF16).astype(F32)
    query = rotate(query).astype(BF16)
    qbuf[me] = query

    pl.semaphore_wait(barrier, N - 1)
    home = lax.shift_right_logical(me, 2)
    for peer in peers:
        send(0, qbuf.at[me], qbuf.at[me], q_sem.at[home], peer)
    lax.fori_loop(0, N, load_weights, 0)

    l_wk.wait()
    l_wv.wait()
    key_part = dot_rows(normed, wk[...]).astype(BF16)
    value_part = dot_rows(normed, wv[...]).astype(BF16)
    quarter = HEAD_DIM // GROUP
    place = lax.broadcasted_iota(jnp.int32, (quarter, HEAD_DIM), 1)
    origin = lax.broadcasted_iota(jnp.int32, (quarter, HEAD_DIM), 0)
    member = jnp.bitwise_and(me, GROUP - 1)
    spread = jnp.where(place == origin + member * quarter, 1.0, 0.0).astype(BF16)
    kvbuf[0, 0] = jnp.dot(key_part, spread, preferred_element_type=F32).astype(BF16)
    kvbuf[0, 1] = jnp.dot(value_part, spread, preferred_element_type=F32).astype(BF16)
    for k in range(1, GROUP):
        peer = me - member + jnp.bitwise_and(member + k, GROUP - 1)
        send(5, kvbuf.at[0], kvbuf.at[k], kv_sem.at[0], peer)

    rows = GROUP * seqs
    row4 = lax.broadcasted_iota(jnp.int32, (rows, HEAD_DIM), 0)
    pick = [jnp.where(lax.rem(row4, seqs) == s, 1.0, 0.0).astype(BF16) for s in range(seqs)]
    valid4 = jnp.concatenate([valid] * GROUP, axis=0)
    lane4 = lax.rem(lax.broadcasted_iota(jnp.int32, (rows, HEAD_DIM), 1), 4)

    def attend(g):
        qg = qbuf[pl.ds(g * GROUP, GROUP)].reshape(rows, HEAD_DIM)
        left = jnp.concatenate([qg * pick[s] for s in range(seqs)], axis=1)
        keys = jnp.concatenate([kc[g, s] for s in range(seqs)], axis=1)
        scores = dot_rows(left, keys)
        scores = jnp.where(valid4, scores * (1.0 / math.sqrt(HEAD_DIM)), LOW)
        top = jnp.max(scores, axis=-1, keepdims=True)
        weights = jnp.where(valid4, jnp.exp(scores - top), 0.0)
        total = row_sum(weights)
        low = weights.astype(BF16)
        left = jnp.concatenate([low * pick[s] for s in range(seqs)], axis=1)
        values = vc[g].reshape(seqs * slots, HEAD_DIM)
        summed = jnp.dot(left, values, preferred_element_type=F32)
        any_slot = total > 0.0
        safe = jnp.where(any_slot, total, 1.0)
        share = (summed * (1.0 / safe)).astype(BF16)
        level = jnp.broadcast_to(jnp.where(any_slot, top + jnp.log(safe), LOW), (rows, HEAD_DIM))
        high, mid, low3 = split3(level)
        stat = jnp.where(
            lane4 == 0, high.astype(F32),
            jnp.where(lane4 == 1, mid.astype(F32), jnp.where(lane4 == 2, low3.astype(F32), 0.0)),
        ).astype(BF16)
        osend[pl.ds(g * GROUP, GROUP), 0] = share.reshape(GROUP, seqs, HEAD_DIM)
        osend[pl.ds(g * GROUP, GROUP), 1] = stat.reshape(GROUP, seqs, HEAD_DIM)

    side = lax.shift_right_logical(z, 2)
    sides = [side, 1 - side]

    def group_at(dy, ds):
        return lax.shift_right_logical(rows_at[dy], 2) + sides[ds]

    loaded(0, kc)
    loaded(1, vc)
    for batch in BATCHES:
        for dy, ds in batch:
            g = group_at(dy, ds)
            arrived(q_sem.at[g], some(qbuf, GROUP - 1 if (dy, ds) == (0, 0) else GROUP))
        for dy, ds in batch:
            attend(group_at(dy, ds))
        for dy, ds in reversed(batch):
            for j in range(GROUP):
                if (dy, ds) == (0, 0):
                    if j == 0:
                        continue
                    peer = me - member + jnp.bitwise_and(member + j, GROUP - 1)
                else:
                    peer = group_at(dy, ds) * GROUP + j
                send(1, osend.at[peer], orecv.at[me], o_sem.at[home], peer)
    sent(0, some(qbuf, N - 1))

    arrived(kv_sem.at[0], some(kvbuf, GROUP - 1))
    key_raw = kvbuf[0, 0].astype(F32)
    value_new = kvbuf[0, 1].astype(F32)
    for k in range(1, GROUP):
        key_raw = key_raw + kvbuf[k, 0].astype(F32)
        value_new = value_new + kvbuf[k, 1].astype(F32)
    key_new = rotate(key_raw).astype(BF16).astype(F32)
    own = row_sum(qbuf[me].astype(F32) * key_new) * (1.0 / math.sqrt(HEAD_DIM))
    own = jnp.broadcast_to(own, (seqs, HEAD_DIM))
    for i, (_, ref) in enumerate(weights):
        loaded(2 + i, ref)
    l_mgain.wait()
    mgain_wide[...] = mgain[...].astype(F32)

    def level_of(stat):
        pair = stat + pltpu.roll(stat, 1, 1)
        return pair + pltpu.roll(pair, 2, 1)

    def merge(state, parts):
        peak, weight_sum, number = state
        levels = [level_of(ref[1].astype(F32)) for ref in parts]
        top = peak
        for level in levels:
            top = jnp.maximum(top, level)
        factor = jnp.exp(peak - top)
        weight_sum = weight_sum * factor
        number = number * factor
        for level, ref in zip(levels, parts):
            factor = jnp.exp(level - top)
            weight_sum = weight_sum + factor
            number = number + factor * ref[0].astype(F32)
        return top, weight_sum, number

    state = merge((own, jnp.ones((seqs, HEAD_DIM), F32), value_new), [osend.at[me]])
    for batch in BATCHES:
        parts = []
        for dy, ds in batch:
            g = group_at(dy, ds)
            if (dy, ds) == (0, 0):
                arrived(o_sem.at[g], some(orecv, GROUP - 1))
                parts += [orecv.at[me - member + jnp.bitwise_and(member + k, GROUP - 1)] for k in range(1, GROUP)]
            else:
                arrived(o_sem.at[g], some(orecv, GROUP))
                parts += [orecv.at[g * GROUP + j] for j in range(GROUP)]
        state = merge(state, parts)
    sent(1, some(osend, N - 1))
    sent(5, some(kvbuf, GROUP - 1))
    attended = (state[2] / state[1]).astype(BF16)

    def scatter(phase, left, weight, stage, landing, recv_sem):
        order = peers + [me]
        far = [d > NEAR for d in DISTANCE] + [False]
        for first in range(0, N, 8):
            part_of = order[first : first + 8]
            for p in part_of:
                stage[p] = jnp.dot(left, weight[p], preferred_element_type=F32).astype(BF16)
            for i, p in enumerate(part_of, first):
                if i < N - 1:
                    send(phase, stage.at[p], landing.at[me], recv_sem.at[int(far[i])], p)

    def gathered(stage, landing, recv_sem):
        total = stage[me].astype(F32)
        for i, (least, most) in enumerate(((1, NEAR), (NEAR + 1, NY + NZ))):
            near = at_distance(least, most)
            arrived(recv_sem.at[i], some(landing, len(near)))
            parts = [landing[p].astype(F32) for p in near]
            while len(parts) > 1:
                parts = [sum(parts[j : j + 2]) for j in range(0, len(parts), 2)]
            total = total + parts[0]
        return total

    scatter(2, attended, wo, psend, precv, p_sem)
    mid_own = (hidden[:, block(me)].astype(F32) + gathered(psend, precv, p_sem)).astype(BF16)
    midbuf[me] = mid_own
    for peer, d in zip(peers, DISTANCE):
        send(3, midbuf.at[me], midbuf.at[me], m_sem.at[mid_class(d)], peer)
    sent(2, some(psend, N - 1))

    squares = jnp.zeros((seqs, 128), F32)
    gate = jnp.zeros((seqs, wg.shape[1]), F32)
    upper = jnp.zeros((seqs, wg.shape[1]), F32)
    for i, (least, most) in enumerate(MID_CLASSES):
        near = at_distance(least, most)
        arrived(m_sem.at[i], some(midbuf, len(near)))
        if i == 0:
            near = near + [me]
        parts = []
        for peer in near:
            part = midbuf[peer].astype(F32)
            squares = squares + part * part
            parts.append((part * mgain_wide[pl.ds(peer, 1), :]).astype(BF16))
        left = jnp.concatenate(parts, axis=1)
        gate = gate + dot_rows(left, jnp.concatenate([wg[p] for p in near], axis=1))
        upper = upper + dot_rows(left, jnp.concatenate([wu[p] for p in near], axis=1))
    scale = lax.rsqrt(row_sum(squares) / width + 1e-5)
    gate = gate * scale
    act = (gate / (1.0 + jnp.exp(-gate)) * (upper * scale)).astype(BF16)
    scatter(4, act, wd, dsend, drecv, d_sem)
    sent(3, some(midbuf, N - 1))
    total = gathered(dsend, drecv, d_sem)
    out_ref[...] = (mid_own.astype(F32) + total).astype(BF16)
    sent(4, some(dsend, N - 1))


def per_device(*args):
    (hidden_in, attn_gain, w_query, w_key, w_value, key_cache, value_cache, write_pos, cache_len, w_out, mlp_gain,
     w_gate, w_up, w_down) = args
    seqs, width = hidden_in.shape
    lines = width // 128
    attn_gain = attn_gain.reshape(lines, 128)
    mlp_gain = mlp_gain.reshape(lines, 128)
    w_key, w_value, w_gate, w_up = w_key.T, w_value.T, w_gate.T, w_up.T
    operands = (hidden_in, attn_gain, w_query, w_key, w_value, key_cache, value_cache, write_pos, cache_len, w_out,
                mlp_gain, w_gate, w_up, w_down)
    held = [pltpu.VMEM(a.shape, a.dtype) for a in operands]
    held[7] = pltpu.SMEM(write_pos.shape, write_pos.dtype)
    held[8] = pltpu.SMEM(cache_len.shape, cache_len.dtype)
    for i in (5, 6):
        held[i] = pltpu.VMEM((KV_HEADS, *key_cache.shape[:2], HEAD_DIM), key_cache.dtype)
    for i in (9, 11, 12, 13):
        held[i] = pltpu.VMEM((lines, operands[i].shape[0], 128), operands[i].dtype)
    block = (N, seqs, 128)
    return pl.pallas_call(
        kernel,
        out_shape=jax.ShapeDtypeStruct((seqs, 128), BF16),
        in_specs=[pl.BlockSpec(memory_space=pltpu.HBM)] * len(operands),
        out_specs=pl.BlockSpec(memory_space=pltpu.VMEM),
        scratch_shapes=held
        + [
            pltpu.VMEM(block, BF16),
            pltpu.VMEM((GROUP, 2, seqs, 128), BF16),
            pltpu.VMEM((N, 2, seqs, 128), BF16),
            pltpu.VMEM((N, 2, seqs, 128), BF16),
            pltpu.VMEM(block, BF16),
            pltpu.VMEM(block, BF16),
            pltpu.VMEM(block, BF16),
            pltpu.VMEM(block, BF16),
            pltpu.VMEM(block, BF16),
            pltpu.VMEM((lines, 128), F32),
            pltpu.SemaphoreType.DMA((len(operands),)),
            pltpu.SemaphoreType.DMA((6,)),
            pltpu.SemaphoreType.DMA((KV_HEADS,)),
            pltpu.SemaphoreType.DMA((1,)),
            pltpu.SemaphoreType.DMA((KV_HEADS,)),
            pltpu.SemaphoreType.DMA((2,)),
            pltpu.SemaphoreType.DMA((len(MID_CLASSES),)),
            pltpu.SemaphoreType.DMA((2,)),
        ],
        compiler_params=pltpu.CompilerParams(
            collective_id=0, has_side_effects=True, vmem_limit_bytes=67043328
        ),
    )(*operands)


def solution(mesh):
    in_specs = (
        P("batch", None),
        P(),
        P(None, "cache"),
        P(None, "cache"),
        P(None, "cache"),
        P("batch", "cache", None),
        P("batch", "cache", None),
        P("batch"),
        P("batch"),
        P("cache", None),
        P(),
        P(None, "cache"),
        P(None, "cache"),
        P("cache", None),
    )
    return jax.shard_map(
        per_device, mesh=mesh, in_specs=in_specs, out_specs=P("batch", "cache"), check_vma=False
    )
```

```python
import functools
import math

import jax
import jax.numpy as jnp
from jax import lax
from jax.experimental import pallas as pl
from jax.experimental.pallas import tpu as pltpu
from jax.sharding import PartitionSpec as P

HEADS = 32
KV_HEADS = 8
HEAD_DIM = 128
GROUP = HEADS // KV_HEADS
NY, NZ = 4, 8
N = NY * NZ
LOW = -1e30
MESH = pl.DeviceIdType.MESH
F32 = jnp.float32
BF16 = jnp.bfloat16

OFFSETS = sorted(
    [(dy, dz) for dy in range(NY) for dz in range(NZ) if (dy, dz) != (0, 0)],
    key=lambda t: -(min(t[0], NY - t[0]) + min(t[1], NZ - t[1])),
)
DISTANCE = [min(dy, NY - dy) + min(dz, NZ - dz) for dy, dz in OFFSETS]
NEAR = 4
PAIRS = sorted(
    [(dy, dz) for dy in range(NY) for dz in range(NZ // 2)],
    key=lambda t: -(min(t[0], NY - t[0]) + max(t[1], NZ // 2 - t[1])),
)
MID_OFFSETS = sorted(
    [(dy, dz) for dy in range(NY) for dz in (7, 0, 1, 2) if (dy, dz) != (0, 0)],
    key=lambda t: -(min(t[0], NY - t[0]) + min(t[1], NZ - t[1])),
)
MID_DISTANCE = [min(dy, NY - dy) + min(dz, NZ - dz) for dy, dz in MID_OFFSETS]
MID_CLASSES = ((1, 2), (3, 3), (4, 4))


def mid_class(distance):
    return [least <= distance <= most for least, most in MID_CLASSES].index(True)


def row_sum(x):
    return jnp.sum(x, axis=-1, keepdims=True)


def dot_rows(a, b):
    return lax.dot_general(a, b, (((1,), (1,)), ((), ())), preferred_element_type=F32)


def split3(x):
    high = x.astype(BF16)
    rest = x - high.astype(F32)
    mid = rest.astype(BF16)
    low = (rest - mid.astype(F32)).astype(BF16)
    return high, mid, low


def kernel(
    hidden_hbm, gain_hbm, wq_hbm, wk_hbm, wv_hbm, kc_hbm, vc_hbm, pos_hbm, len_hbm,
    wo_hbm, mgain_hbm, wg_hbm, wu_hbm, wd_hbm,
    out_ref,
    hidden, gain, wq, wk, wv, kc, vc, pos_ref, len_ref, wo, mgain, wg, wu, wd,
    qbuf, kvbuf, osend, orecv, psend, precv, midbuf, dsend, drecv, mgain_wide, ktr, wgt, wut,
    load_sem, send_sem, q_sem, kv_sem, o_sem, p_sem, m_sem, d_sem,
):
    me = lax.axis_index("cache")
    y, z = lax.shift_right_logical(me, 3), jnp.bitwise_and(me, NZ - 1)
    seqs = hidden.shape[0]
    width = hidden.shape[1]
    slots = kc.shape[2]

    rows_at = [jnp.bitwise_and(y + dy, NY - 1) * NZ for dy in range(NY)]
    cols_at = [jnp.bitwise_and(z + dz, NZ - 1) for dz in range(NZ)]
    peers = [rows_at[dy] + cols_at[dz] for dy, dz in OFFSETS]

    def at_distance(least, most):
        return [p for p, d in zip(peers, DISTANCE) if least <= d <= most]

    barrier = pltpu.get_barrier_semaphore()
    for peer in peers:
        pl.semaphore_signal(barrier, inc=1, device_id={"cache": peer}, device_id_type=MESH)

    def block(c):
        return pl.ds(pl.multiple_of(c * 128, 128), 128)

    plain = [
        (hidden_hbm, hidden), (gain_hbm, gain), (pos_hbm, pos_ref), (len_hbm, len_ref), (wq_hbm, wq), (wk_hbm, wk),
        (wv_hbm, wv), (mgain_hbm, mgain),
    ]
    loads = [pltpu.make_async_copy(a, b, load_sem.at[i]) for i, (a, b) in enumerate(plain)]
    for copy in loads:
        copy.start()
    l_hidden, l_gain, l_pos, l_len, l_wq, l_wk, l_wv, l_mgain = loads
    first = len(plain)
    for g in range(KV_HEADS):
        pltpu.make_async_copy(kc_hbm.at[:, :, block(g)], kc.at[g], load_sem.at[first]).start()
    for g in range(KV_HEADS):
        pltpu.make_async_copy(vc_hbm.at[:, :, block(g)], vc.at[g], load_sem.at[first + 1]).start()
    weights = ((wo_hbm, wo), (wg_hbm, wg), (wu_hbm, wu), (wd_hbm, wd))

    def load_weights(c, _):
        for i, (a, b) in enumerate(weights):
            pltpu.make_async_copy(a.at[:, block(c)], b.at[c], load_sem.at[first + 2 + i]).start()
        return 0

    def loaded(i, ref):
        pltpu.make_async_copy(ref, ref, load_sem.at[first + i]).wait()

    def send(phase, src, dst, recv_sem, peer):
        pltpu.make_async_remote_copy(
            src_ref=src, dst_ref=dst, send_sem=send_sem.at[phase], recv_sem=recv_sem,
            device_id={"cache": peer}, device_id_type=MESH,
        ).start()

    def pending(phase, ref, recv_sem):
        return pltpu.make_async_remote_copy(
            src_ref=ref, dst_ref=ref, send_sem=send_sem.at[phase], recv_sem=recv_sem,
            device_id={"cache": peers[0]}, device_id_type=MESH,
        )

    def arrived(recv_sem, ref):
        pending(0, ref, recv_sem).wait_recv()

    def sent(phase, ref):
        pending(phase, ref, kv_sem.at[0]).wait_send()

    def some(buffer, count):
        return buffer.at[pl.ds(0, count)]

    lane = lax.broadcasted_iota(jnp.int32, (seqs, HEAD_DIM), 1)
    row = lax.broadcasted_iota(jnp.int32, (seqs, HEAD_DIM), 0)
    half = HEAD_DIM // 2
    l_pos.wait()
    l_len.wait()
    pos = jnp.zeros((seqs, HEAD_DIM), jnp.int32)
    length = jnp.zeros((seqs, HEAD_DIM), jnp.int32)
    for s in range(seqs):
        pos = jnp.where(row == s, pos_ref[s], pos)
        length = jnp.where(row == s, len_ref[s], length)
    freq = jnp.exp(lax.rem(lane, half).astype(F32) * (-math.log(10000.0) / half))
    angle = pos.astype(F32) * freq
    cosine = jnp.cos(angle)
    sine = jnp.sin(angle) * jnp.where(lane < half, -1.0, 1.0)

    def rotate(x):
        return x * cosine + pltpu.roll(x, half, 1) * sine

    slot = me * slots + lane
    dist = jnp.bitwise_and(pos - 1 - slot, slots * N - 1) + 1
    valid = dist <= length

    l_hidden.wait()
    l_gain.wait()
    wide = hidden[...].astype(F32)
    scale = lax.rsqrt(row_sum(wide * wide) / width + 1e-5)
    chunks = []
    for c in range(width // 128):
        part = wide[:, c * 128 : (c + 1) * 128] * scale * gain[c : c + 1, :].astype(F32)
        chunks.append(part.astype(BF16))
    normed = jnp.concatenate(chunks, axis=1)
    l_wq.wait()
    query = jnp.dot(normed, wq[...], preferred_element_type=F32).astype(BF16).astype(F32)
    query = rotate(query).astype(BF16)
    qbuf[me] = query

    pl.semaphore_wait(barrier, N - 1)
    for peer in peers:
        send(0, qbuf.at[me], qbuf.at[me], q_sem.at[0], peer)
    lax.fori_loop(0, N, load_weights, 0)

    l_wk.wait()
    l_wv.wait()
    key_part = dot_rows(normed, wk[...]).astype(BF16)
    value_part = dot_rows(normed, wv[...]).astype(BF16)
    quarter = HEAD_DIM // GROUP
    place = lax.broadcasted_iota(jnp.int32, (quarter, HEAD_DIM), 1)
    origin = lax.broadcasted_iota(jnp.int32, (quarter, HEAD_DIM), 0)
    member = jnp.bitwise_and(me, GROUP - 1)
    spread = jnp.where(place == origin + member * quarter, 1.0, 0.0).astype(BF16)
    kvbuf[0, 0] = jnp.dot(key_part, spread, preferred_element_type=F32).astype(BF16)
    kvbuf[0, 1] = jnp.dot(value_part, spread, preferred_element_type=F32).astype(BF16)
    for k in range(1, GROUP):
        peer = me - member + jnp.bitwise_and(member + k, GROUP - 1)
        send(5, kvbuf.at[0], kvbuf.at[k], kv_sem.at[0], peer)

    rows = GROUP * seqs
    row4 = lax.broadcasted_iota(jnp.int32, (rows, HEAD_DIM), 0)
    pick = [jnp.where(lax.rem(row4, seqs) == s, 1.0, 0.0).astype(BF16) for s in range(seqs)]
    valid4 = jnp.concatenate([valid] * GROUP, axis=0)
    lane4 = lax.rem(lax.broadcasted_iota(jnp.int32, (rows, HEAD_DIM), 1), 4)

    def attend(groups):
        scores = []
        for g in groups:
            qg = qbuf[pl.ds(g * GROUP, GROUP)].reshape(rows, HEAD_DIM)
            left = jnp.concatenate([qg * pick[s] for s in range(seqs)], axis=1)
            keys = ktr[g].reshape(seqs * HEAD_DIM, slots)
            scores.append(jnp.dot(left, keys, preferred_element_type=F32))
        shares, tops, totals = [], [], []
        for score in scores:
            score = jnp.where(valid4, score * (1.0 / math.sqrt(HEAD_DIM)), LOW)
            top = jnp.max(score, axis=-1, keepdims=True)
            weights = jnp.where(valid4, jnp.exp(score - top), 0.0)
            tops.append(top)
            totals.append(row_sum(weights))
            shares.append(weights.astype(BF16))
        for g, low, top, total in zip(groups, shares, tops, totals):
            left = jnp.concatenate([low * pick[s] for s in range(seqs)], axis=1)
            values = vc[g].reshape(seqs * slots, HEAD_DIM)
            summed = jnp.dot(left, values, preferred_element_type=F32)
            any_slot = total > 0.0
            safe = jnp.where(any_slot, total, 1.0)
            share = (summed * (1.0 / safe)).astype(BF16)
            level = jnp.broadcast_to(jnp.where(any_slot, top + jnp.log(safe), LOW), (rows, HEAD_DIM))
            high, mid, low3 = split3(level)
            stat = jnp.where(
                lane4 == 0, high.astype(F32),
                jnp.where(lane4 == 1, mid.astype(F32), jnp.where(lane4 == 2, low3.astype(F32), 0.0)),
            ).astype(BF16)
            osend[pl.ds(g * GROUP, GROUP), 0] = share.reshape(GROUP, seqs, HEAD_DIM)
            osend[pl.ds(g * GROUP, GROUP), 1] = stat.reshape(GROUP, seqs, HEAD_DIM)

    loaded(0, kc)
    loaded(1, vc)

    def turn_keys(g, _):
        for s in range(seqs):
            ktr[g, s] = kc[g, s].T
        return 0

    lax.fori_loop(0, KV_HEADS, turn_keys, 0)
    arrived(q_sem.at[0], some(qbuf, N - 1))
    attend(range(KV_HEADS))
    for peer, d in zip(peers, DISTANCE):
        send(1, osend.at[peer], orecv.at[me], o_sem.at[int(d > NEAR)], peer)
    sent(0, some(qbuf, N - 1))

    arrived(kv_sem.at[0], some(kvbuf, GROUP - 1))
    key_raw = kvbuf[0, 0].astype(F32)
    value_new = kvbuf[0, 1].astype(F32)
    for k in range(1, GROUP):
        key_raw = key_raw + kvbuf[k, 0].astype(F32)
        value_new = value_new + kvbuf[k, 1].astype(F32)
    key_new = rotate(key_raw).astype(BF16).astype(F32)
    own = row_sum(qbuf[me].astype(F32) * key_new) * (1.0 / math.sqrt(HEAD_DIM))
    own = jnp.broadcast_to(own, (seqs, HEAD_DIM))
    for i, (_, ref) in enumerate(weights):
        loaded(2 + i, ref)
    l_mgain.wait()

    def turn_weights(c, _):
        wgt[c] = wg[c].T
        wut[c] = wu[c].T
        return 0

    lax.fori_loop(0, N, turn_weights, 0)
    mgain_wide[...] = mgain[...].astype(F32)

    def level_of(stat):
        pair = stat + pltpu.roll(stat, 1, 1)
        return pair + pltpu.roll(pair, 2, 1)

    def merge(state, parts):
        peak, weight_sum, number = state
        levels = [level_of(ref[1].astype(F32)) for ref in parts]
        top = peak
        for level in levels:
            top = jnp.maximum(top, level)
        factor = jnp.exp(peak - top)
        weight_sum = weight_sum * factor
        number = number * factor
        for level, ref in zip(levels, parts):
            factor = jnp.exp(level - top)
            weight_sum = weight_sum + factor
            number = number + factor * ref[0].astype(F32)
        return top, weight_sum, number

    state = merge((own, jnp.ones((seqs, HEAD_DIM), F32), value_new), [osend.at[me]])
    for i, (least, most) in enumerate(((1, NEAR), (NEAR + 1, NY + NZ))):
        near = at_distance(least, most)
        arrived(o_sem.at[i], some(orecv, len(near)))
        state = merge(state, [orecv.at[p] for p in near])
    sent(1, some(osend, N - 1))
    sent(5, some(kvbuf, GROUP - 1))
    attended = (state[2] / state[1]).astype(BF16)

    def scatter(phase, left, weight, stage, landing, recv_sem):
        order = peers + [me]
        far = [d > NEAR for d in DISTANCE] + [False]
        for first in range(0, N, 8):
            part_of = order[first : first + 8]
            for p in part_of:
                stage[p] = jnp.dot(left, weight[p], preferred_element_type=F32).astype(BF16)
            for i, p in enumerate(part_of, first):
                if i < N - 1:
                    send(phase, stage.at[p], landing.at[me], recv_sem.at[int(far[i])], p)

    def gathered(stage, landing, recv_sem):
        total = stage[me].astype(F32)
        for i, (least, most) in enumerate(((1, NEAR), (NEAR + 1, NY + NZ))):
            near = at_distance(least, most)
            arrived(recv_sem.at[i], some(landing, len(near)))
            parts = [landing[p].astype(F32) for p in near]
            while len(parts) > 1:
                parts = [sum(parts[j : j + 2]) for j in range(0, len(parts), 2)]
            total = total + parts[0]
        return total

    def tree(parts):
        while len(parts) > 1:
            parts = [sum(parts[j : j + 2]) for j in range(0, len(parts), 2)]
        return parts[0]

    quad = jnp.bitwise_and(z, NZ // 2 - 1)
    mine = lax.shift_right_logical(rows_at[0], 1) + quad
    for first in range(0, len(PAIRS), 4):
        part_of = PAIRS[first : first + 4]
        for dy, dz in part_of:
            column = rows_at[dy] + jnp.bitwise_and(z + dz, NZ // 2 - 1)
            at = psend.at[lax.shift_right_logical(rows_at[dy], 1) + jnp.bitwise_and(z + dz, NZ // 2 - 1)]
            for h in range(2):
                part = jnp.dot(attended, wo[column + h * (NZ // 2)], preferred_element_type=F32).astype(BF16)
                at[h] = part
                if (dy, dz) == (0, 0):
                    precv[me, h] = part
        for dy, dz in part_of:
            at = psend.at[lax.shift_right_logical(rows_at[dy], 1) + jnp.bitwise_and(z + dz, NZ // 2 - 1)]
            for far in (dz, dz + NZ // 2):
                if (dy, far) != (0, 0):
                    send(2, at, precv.at[me], p_sem.at[0], rows_at[dy] + cols_at[far])

    arrived(p_sem.at[0], some(precv, N - 1))
    for h in range(2):
        total = tree([precv[j, h].astype(F32) for j in range(N)])
        column = block(rows_at[0] + quad + h * (NZ // 2))
        midbuf[mine, h] = (hidden[:, column].astype(F32) + total).astype(BF16)
    for (dy, dz), d in zip(MID_OFFSETS, MID_DISTANCE):
        send(3, midbuf.at[mine], midbuf.at[mine], m_sem.at[mid_class(d)], rows_at[dy] + cols_at[dz])
    sent(2, some(precv, N - 1))

    squares = jnp.zeros((seqs, 128), F32)
    gate = jnp.zeros((seqs, wg.shape[1]), F32)
    upper = jnp.zeros((seqs, wg.shape[1]), F32)
    for i, (least, most) in enumerate(MID_CLASSES):
        near = [(-dy % NY, -dz % NZ) for (dy, dz), d in zip(MID_OFFSETS, MID_DISTANCE) if least <= d <= most]
        arrived(m_sem.at[i], some(midbuf, len(near)))
        if i == 0:
            near = near + [(0, 0)]
        parts, columns = [], []
        for dy, dz in near:
            low_z = jnp.bitwise_and(z + dz, NZ // 2 - 1)
            pair = lax.shift_right_logical(rows_at[dy], 1) + low_z
            for h in range(2):
                column = rows_at[dy] + low_z + h * (NZ // 2)
                part = midbuf[pair, h].astype(F32)
                squares = squares + part * part
                parts.append((part * mgain_wide[pl.ds(column, 1), :]).astype(BF16))
                columns.append(column)
        left = jnp.concatenate(parts, axis=1)
        gate = gate + jnp.dot(left, jnp.concatenate([wgt[p] for p in columns], axis=0), preferred_element_type=F32)
        upper = upper + jnp.dot(left, jnp.concatenate([wut[p] for p in columns], axis=0), preferred_element_type=F32)
    scale = lax.rsqrt(row_sum(squares) / width + 1e-5)
    gate = gate * scale
    act = (gate / (1.0 + jnp.exp(-gate)) * (upper * scale)).astype(BF16)
    scatter(4, act, wd, dsend, drecv, d_sem)
    sent(3, some(midbuf, len(MID_OFFSETS)))
    total = gathered(dsend, drecv, d_sem)
    mid_own = midbuf[mine, lax.shift_right_logical(z, 2)]
    out_ref[...] = (mid_own.astype(F32) + total).astype(BF16)
    sent(4, some(dsend, N - 1))


def per_device(*args):
    (hidden_in, attn_gain, w_query, w_key, w_value, key_cache, value_cache, write_pos, cache_len, w_out, mlp_gain,
     w_gate, w_up, w_down) = args
    seqs, width = hidden_in.shape
    lines = width // 128
    attn_gain = attn_gain.reshape(lines, 128)
    mlp_gain = mlp_gain.reshape(lines, 128)
    w_key, w_value, w_gate, w_up = w_key.T, w_value.T, w_gate.T, w_up.T
    operands = (hidden_in, attn_gain, w_query, w_key, w_value, key_cache, value_cache, write_pos, cache_len, w_out,
                mlp_gain, w_gate, w_up, w_down)
    held = [pltpu.VMEM(a.shape, a.dtype) for a in operands]
    held[7] = pltpu.SMEM(write_pos.shape, write_pos.dtype)
    held[8] = pltpu.SMEM(cache_len.shape, cache_len.dtype)
    for i in (5, 6):
        held[i] = pltpu.VMEM((KV_HEADS, *key_cache.shape[:2], HEAD_DIM), key_cache.dtype)
    for i in (9, 11, 12, 13):
        held[i] = pltpu.VMEM((lines, operands[i].shape[0], 128), operands[i].dtype)
    block = (N, seqs, 128)
    return pl.pallas_call(
        kernel,
        out_shape=jax.ShapeDtypeStruct((seqs, 128), BF16),
        in_specs=[pl.BlockSpec(memory_space=pltpu.HBM)] * len(operands),
        out_specs=pl.BlockSpec(memory_space=pltpu.VMEM),
        scratch_shapes=held
        + [
            pltpu.VMEM(block, BF16),
            pltpu.VMEM((GROUP, 2, seqs, 128), BF16),
            pltpu.VMEM((N, 2, seqs, 128), BF16),
            pltpu.VMEM((N, 2, seqs, 128), BF16),
            pltpu.VMEM((N // 2, 2, seqs, 128), BF16),
            pltpu.VMEM((N, 2, seqs, 128), BF16),
            pltpu.VMEM((N // 2, 2, seqs, 128), BF16),
            pltpu.VMEM(block, BF16),
            pltpu.VMEM(block, BF16),
            pltpu.VMEM((lines, 128), F32),
            pltpu.VMEM((KV_HEADS, seqs, HEAD_DIM, key_cache.shape[1]), BF16),
            pltpu.VMEM((lines, 128, w_gate.shape[0]), BF16),
            pltpu.VMEM((lines, 128, w_up.shape[0]), BF16),
            pltpu.SemaphoreType.DMA((len(operands),)),
            pltpu.SemaphoreType.DMA((6,)),
            pltpu.SemaphoreType.DMA((1,)),
            pltpu.SemaphoreType.DMA((1,)),
            pltpu.SemaphoreType.DMA((2,)),
            pltpu.SemaphoreType.DMA((1,)),
            pltpu.SemaphoreType.DMA((len(MID_CLASSES),)),
            pltpu.SemaphoreType.DMA((2,)),
        ],
        compiler_params=pltpu.CompilerParams(
            collective_id=0, has_side_effects=True, vmem_limit_bytes=67043328
        ),
    )(*operands)


def solution(mesh):
    in_specs = (
        P("batch", None),
        P(),
        P(None, "cache"),
        P(None, "cache"),
        P(None, "cache"),
        P("batch", "cache", None),
        P("batch", "cache", None),
        P("batch"),
        P("batch"),
        P("cache", None),
        P(),
        P(None, "cache"),
        P(None, "cache"),
        P("cache", None),
    )
    return jax.shard_map(
        per_device, mesh=mesh, in_specs=in_specs, out_specs=P("batch", "cache"), check_vma=False
    )
```

```python
import functools
import math

import jax
import jax.numpy as jnp
from jax import lax
from jax.experimental import pallas as pl
from jax.experimental.pallas import tpu as pltpu
from jax.sharding import PartitionSpec as P

HEADS = 32
KV_HEADS = 8
HEAD_DIM = 128
GROUP = HEADS // KV_HEADS
NY, NZ = 4, 8
N = NY * NZ
LOW = -1e30
MESH = pl.DeviceIdType.MESH
F32 = jnp.float32
BF16 = jnp.bfloat16

OFFSETS = sorted(
    [(dy, dz) for dy in range(NY) for dz in range(NZ) if (dy, dz) != (0, 0)],
    key=lambda t: -(min(t[0], NY - t[0]) + min(t[1], NZ - t[1])),
)
DISTANCE = [min(dy, NY - dy) + min(dz, NZ - dz) for dy, dz in OFFSETS]
NEAR = 4
PAIRS = sorted(
    [(dy, dz) for dy in range(NY) for dz in range(NZ // 2)],
    key=lambda t: -(min(t[0], NY - t[0]) + max(t[1], NZ // 2 - t[1])),
)
MID_OFFSETS = sorted(
    [(dy, dz) for dy in range(NY) for dz in (7, 0, 1, 2) if (dy, dz) != (0, 0)],
    key=lambda t: -(min(t[0], NY - t[0]) + min(t[1], NZ - t[1])),
)
MID_DISTANCE = [min(dy, NY - dy) + min(dz, NZ - dz) for dy, dz in MID_OFFSETS]
MID_CLASSES = ((1, 1), (2, 2), (3, 3), (4, 4))


def mid_class(distance):
    return [least <= distance <= most for least, most in MID_CLASSES].index(True)


def row_sum(x):
    return jnp.sum(x, axis=-1, keepdims=True)


def dot_rows(a, b):
    return lax.dot_general(a, b, (((1,), (1,)), ((), ())), preferred_element_type=F32)


def split3(x):
    high = x.astype(BF16)
    rest = x - high.astype(F32)
    mid = rest.astype(BF16)
    low = (rest - mid.astype(F32)).astype(BF16)
    return high, mid, low


def kernel(
    hidden_hbm, gain_hbm, wq_hbm, wk_hbm, wv_hbm, kc_hbm, vc_hbm, pos_hbm, len_hbm,
    wo_hbm, mgain_hbm, wg_hbm, wu_hbm, wd_hbm,
    out_ref,
    hidden, gain, wq, wk, wv, kc, vc, pos_ref, len_ref, wo, mgain, wg, wu, wd,
    qbuf, kvbuf, osend, orecv, psend, precv, midbuf, dsend, drecv, mgain_wide, ktr, wgt, wut,
    load_sem, send_sem, q_sem, kv_sem, o_sem, p_sem, m_sem, d_sem,
):
    me = lax.axis_index("cache")
    y, z = lax.shift_right_logical(me, 3), jnp.bitwise_and(me, NZ - 1)
    seqs = hidden.shape[0]
    width = hidden.shape[1]
    slots = kc.shape[2]

    rows_at = [jnp.bitwise_and(y + dy, NY - 1) * NZ for dy in range(NY)]
    cols_at = [jnp.bitwise_and(z + dz, NZ - 1) for dz in range(NZ)]
    peers = [rows_at[dy] + cols_at[dz] for dy, dz in OFFSETS]

    def at_distance(least, most):
        return [p for p, d in zip(peers, DISTANCE) if least <= d <= most]

    barrier = pltpu.get_barrier_semaphore()
    for peer in peers:
        pl.semaphore_signal(barrier, inc=1, device_id={"cache": peer}, device_id_type=MESH)

    def block(c):
        return pl.ds(pl.multiple_of(c * 128, 128), 128)

    plain = [
        (hidden_hbm, hidden), (gain_hbm, gain), (pos_hbm, pos_ref), (len_hbm, len_ref), (wq_hbm, wq), (wk_hbm, wk),
        (wv_hbm, wv), (mgain_hbm, mgain),
    ]
    loads = [pltpu.make_async_copy(a, b, load_sem.at[i]) for i, (a, b) in enumerate(plain)]
    for copy in loads:
        copy.start()
    l_hidden, l_gain, l_pos, l_len, l_wq, l_wk, l_wv, l_mgain = loads
    first = len(plain)
    for g in range(KV_HEADS):
        pltpu.make_async_copy(kc_hbm.at[:, :, block(g)], kc.at[g], load_sem.at[first]).start()
    for g in range(KV_HEADS):
        pltpu.make_async_copy(vc_hbm.at[:, :, block(g)], vc.at[g], load_sem.at[first + 1]).start()
    weights = ((wo_hbm, wo), (wg_hbm, wg), (wu_hbm, wu), (wd_hbm, wd))

    def load_weights(c, _):
        for i, (a, b) in enumerate(weights):
            pltpu.make_async_copy(a.at[:, block(c)], b.at[c], load_sem.at[first + 2 + i]).start()
        return 0

    def loaded(i, ref):
        pltpu.make_async_copy(ref, ref, load_sem.at[first + i]).wait()

    def send(phase, src, dst, recv_sem, peer):
        pltpu.make_async_remote_copy(
            src_ref=src, dst_ref=dst, send_sem=send_sem.at[phase], recv_sem=recv_sem,
            device_id={"cache": peer}, device_id_type=MESH,
        ).start()

    def pending(phase, ref, recv_sem):
        return pltpu.make_async_remote_copy(
            src_ref=ref, dst_ref=ref, send_sem=send_sem.at[phase], recv_sem=recv_sem,
            device_id={"cache": peers[0]}, device_id_type=MESH,
        )

    def arrived(recv_sem, ref):
        pending(0, ref, recv_sem).wait_recv()

    def sent(phase, ref):
        pending(phase, ref, kv_sem.at[0]).wait_send()

    def some(buffer, count):
        return buffer.at[pl.ds(0, count)]

    lane = lax.broadcasted_iota(jnp.int32, (seqs, HEAD_DIM), 1)
    row = lax.broadcasted_iota(jnp.int32, (seqs, HEAD_DIM), 0)
    half = HEAD_DIM // 2
    l_pos.wait()
    l_len.wait()
    pos = jnp.zeros((seqs, HEAD_DIM), jnp.int32)
    length = jnp.zeros((seqs, HEAD_DIM), jnp.int32)
    for s in range(seqs):
        pos = jnp.where(row == s, pos_ref[s], pos)
        length = jnp.where(row == s, len_ref[s], length)
    freq = jnp.exp(lax.rem(lane, half).astype(F32) * (-math.log(10000.0) / half))
    angle = pos.astype(F32) * freq
    cosine = jnp.cos(angle)
    sine = jnp.sin(angle) * jnp.where(lane < half, -1.0, 1.0)

    def rotate(x):
        return x * cosine + pltpu.roll(x, half, 1) * sine

    slot = me * slots + lane
    dist = jnp.bitwise_and(pos - 1 - slot, slots * N - 1) + 1
    valid = dist <= length

    l_hidden.wait()
    l_gain.wait()
    wide = hidden[...].astype(F32)
    scale = lax.rsqrt(row_sum(wide * wide) / width + 1e-5)
    chunks = []
    for c in range(width // 128):
        part = wide[:, c * 128 : (c + 1) * 128] * scale * gain[c : c + 1, :].astype(F32)
        chunks.append(part.astype(BF16))
    normed = jnp.concatenate(chunks, axis=1)
    l_wq.wait()
    query = jnp.dot(normed, wq[...], preferred_element_type=F32).astype(BF16).astype(F32)
    query = rotate(query).astype(BF16)
    qbuf[me] = query

    pl.semaphore_wait(barrier, N - 1)
    for peer in peers:
        send(0, qbuf.at[me], qbuf.at[me], q_sem.at[0], peer)
    lax.fori_loop(0, N, load_weights, 0)

    l_wk.wait()
    l_wv.wait()
    key_part = dot_rows(normed, wk[...]).astype(BF16)
    value_part = dot_rows(normed, wv[...]).astype(BF16)
    quarter = HEAD_DIM // GROUP
    place = lax.broadcasted_iota(jnp.int32, (quarter, HEAD_DIM), 1)
    origin = lax.broadcasted_iota(jnp.int32, (quarter, HEAD_DIM), 0)
    member = jnp.bitwise_and(me, GROUP - 1)
    spread = jnp.where(place == origin + member * quarter, 1.0, 0.0).astype(BF16)
    kvbuf[0, 0] = jnp.dot(key_part, spread, preferred_element_type=F32).astype(BF16)
    kvbuf[0, 1] = jnp.dot(value_part, spread, preferred_element_type=F32).astype(BF16)
    for k in range(1, GROUP):
        peer = me - member + jnp.bitwise_and(member + k, GROUP - 1)
        send(5, kvbuf.at[0], kvbuf.at[k], kv_sem.at[0], peer)

    rows = GROUP * seqs
    row4 = lax.broadcasted_iota(jnp.int32, (rows, HEAD_DIM), 0)
    pick = [jnp.where(lax.rem(row4, seqs) == s, 1.0, 0.0).astype(BF16) for s in range(seqs)]
    valid4 = jnp.concatenate([valid] * GROUP, axis=0)
    lane4 = lax.rem(lax.broadcasted_iota(jnp.int32, (rows, HEAD_DIM), 1), 4)

    def attend(groups):
        scores = []
        for g in groups:
            qg = qbuf[pl.ds(g * GROUP, GROUP)].reshape(rows, HEAD_DIM)
            left = jnp.concatenate([qg * pick[s] for s in range(seqs)], axis=1)
            keys = ktr[g].reshape(seqs * HEAD_DIM, slots)
            scores.append(jnp.dot(left, keys, preferred_element_type=F32))
        shares, tops, totals = [], [], []
        for score in scores:
            score = jnp.where(valid4, score * (1.0 / math.sqrt(HEAD_DIM)), LOW)
            top = jnp.max(score, axis=-1, keepdims=True)
            weights = jnp.where(valid4, jnp.exp(score - top), 0.0)
            tops.append(top)
            totals.append(row_sum(weights))
            shares.append(weights.astype(BF16))
        for g, low, top, total in zip(groups, shares, tops, totals):
            left = jnp.concatenate([low * pick[s] for s in range(seqs)], axis=1)
            values = vc[g].reshape(seqs * slots, HEAD_DIM)
            summed = jnp.dot(left, values, preferred_element_type=F32)
            any_slot = total > 0.0
            safe = jnp.where(any_slot, total, 1.0)
            share = (summed * (1.0 / safe)).astype(BF16)
            level = jnp.broadcast_to(jnp.where(any_slot, top + jnp.log(safe), LOW), (rows, HEAD_DIM))
            high, mid, low3 = split3(level)
            stat = jnp.where(
                lane4 == 0, high.astype(F32),
                jnp.where(lane4 == 1, mid.astype(F32), jnp.where(lane4 == 2, low3.astype(F32), 0.0)),
            ).astype(BF16)
            osend[pl.ds(g * GROUP, GROUP), 0] = share.reshape(GROUP, seqs, HEAD_DIM)
            osend[pl.ds(g * GROUP, GROUP), 1] = stat.reshape(GROUP, seqs, HEAD_DIM)

    loaded(0, kc)
    loaded(1, vc)

    def turn_keys(g, _):
        for s in range(seqs):
            ktr[g, s] = kc[g, s].T
        return 0

    lax.fori_loop(0, KV_HEADS, turn_keys, 0)
    arrived(q_sem.at[0], some(qbuf, N - 1))
    attend(range(KV_HEADS))
    for peer, d in zip(peers, DISTANCE):
        send(1, osend.at[peer], orecv.at[me], o_sem.at[int(d > NEAR)], peer)
    sent(0, some(qbuf, N - 1))

    arrived(kv_sem.at[0], some(kvbuf, GROUP - 1))
    key_raw = kvbuf[0, 0].astype(F32)
    value_new = kvbuf[0, 1].astype(F32)
    for k in range(1, GROUP):
        key_raw = key_raw + kvbuf[k, 0].astype(F32)
        value_new = value_new + kvbuf[k, 1].astype(F32)
    key_new = rotate(key_raw).astype(BF16).astype(F32)
    own = row_sum(qbuf[me].astype(F32) * key_new) * (1.0 / math.sqrt(HEAD_DIM))
    own = jnp.broadcast_to(own, (seqs, HEAD_DIM))
    for i, (_, ref) in enumerate(weights):
        loaded(2 + i, ref)
    l_mgain.wait()

    def turn_weights(c, _):
        wgt[c] = wg[c].T
        wut[c] = wu[c].T
        return 0

    lax.fori_loop(0, N, turn_weights, 0)
    mgain_wide[...] = mgain[...].astype(F32)

    def level_of(stat):
        return (stat + pltpu.roll(stat, 1, 1)) + (pltpu.roll(stat, 2, 1) + pltpu.roll(stat, 3, 1))

    def merge(state, parts):
        peak, weight_sum, number = state
        levels = [level_of(ref[1].astype(F32)) for ref in parts]
        top = peak
        for level in levels:
            top = jnp.maximum(top, level)
        factor = jnp.exp(peak - top)
        weight_sum = weight_sum * factor
        number = number * factor
        for level, ref in zip(levels, parts):
            factor = jnp.exp(level - top)
            weight_sum = weight_sum + factor
            number = number + factor * ref[0].astype(F32)
        return top, weight_sum, number

    state = merge((own, jnp.ones((seqs, HEAD_DIM), F32), value_new), [osend.at[me]])
    for i, (least, most) in enumerate(((1, NEAR), (NEAR + 1, NY + NZ))):
        near = at_distance(least, most)
        arrived(o_sem.at[i], some(orecv, len(near)))
        state = merge(state, [orecv.at[p] for p in near])
    sent(1, some(osend, N - 1))
    sent(5, some(kvbuf, GROUP - 1))
    attended = (state[2] / state[1]).astype(BF16)

    def scatter(phase, left, weight, stage, landing, recv_sem):
        order = peers + [me]
        far = [d > NEAR for d in DISTANCE] + [False]
        for first in range(0, N, 8):
            part_of = order[first : first + 8]
            for p in part_of:
                stage[p] = jnp.dot(left, weight[p], preferred_element_type=F32).astype(BF16)
            for i, p in enumerate(part_of, first):
                if i < N - 1:
                    send(phase, stage.at[p], landing.at[me], recv_sem.at[int(far[i])], p)

    def gathered(stage, landing, recv_sem):
        total = stage[me].astype(F32)
        for i, (least, most) in enumerate(((1, NEAR), (NEAR + 1, NY + NZ))):
            near = at_distance(least, most)
            arrived(recv_sem.at[i], some(landing, len(near)))
            parts = [landing[p].astype(F32) for p in near]
            while len(parts) > 1:
                parts = [sum(parts[j : j + 2]) for j in range(0, len(parts), 2)]
            total = total + parts[0]
        return total

    def tree(parts):
        while len(parts) > 1:
            parts = [sum(parts[j : j + 2]) for j in range(0, len(parts), 2)]
        return parts[0]

    quad = jnp.bitwise_and(z, NZ // 2 - 1)
    mine = lax.shift_right_logical(rows_at[0], 1) + quad
    for first in range(0, len(PAIRS), 4):
        part_of = PAIRS[first : first + 4]
        for dy, dz in part_of:
            column = rows_at[dy] + jnp.bitwise_and(z + dz, NZ // 2 - 1)
            at = psend.at[lax.shift_right_logical(rows_at[dy], 1) + jnp.bitwise_and(z + dz, NZ // 2 - 1)]
            for h in range(2):
                part = jnp.dot(attended, wo[column + h * (NZ // 2)], preferred_element_type=F32).astype(BF16)
                at[h] = part
                if (dy, dz) == (0, 0):
                    precv[me, h] = part
        for dy, dz in part_of:
            at = psend.at[lax.shift_right_logical(rows_at[dy], 1) + jnp.bitwise_and(z + dz, NZ // 2 - 1)]
            for far in (dz, dz + NZ // 2):
                if (dy, far) != (0, 0):
                    send(2, at, precv.at[me], p_sem.at[0], rows_at[dy] + cols_at[far])

    arrived(p_sem.at[0], some(precv, N - 1))
    for h in range(2):
        total = tree([precv[j, h].astype(F32) for j in range(N)])
        column = block(rows_at[0] + quad + h * (NZ // 2))
        midbuf[mine, h] = (hidden[:, column].astype(F32) + total).astype(BF16)
    for (dy, dz), d in zip(MID_OFFSETS, MID_DISTANCE):
        send(3, midbuf.at[mine], midbuf.at[mine], m_sem.at[mid_class(d)], rows_at[dy] + cols_at[dz])
    sent(2, some(precv, N - 1))

    squares = jnp.zeros((seqs, 128), F32)
    gate = jnp.zeros((seqs, wg.shape[1]), F32)
    upper = jnp.zeros((seqs, wg.shape[1]), F32)
    for i, (least, most) in enumerate(MID_CLASSES):
        near = [(-dy % NY, -dz % NZ) for (dy, dz), d in zip(MID_OFFSETS, MID_DISTANCE) if least <= d <= most]
        arrived(m_sem.at[i], some(midbuf, len(near)))
        if i == 0:
            near = near + [(0, 0)]
        parts, columns = [], []
        for dy, dz in near:
            low_z = jnp.bitwise_and(z + dz, NZ // 2 - 1)
            pair = lax.shift_right_logical(rows_at[dy], 1) + low_z
            for h in range(2):
                column = rows_at[dy] + low_z + h * (NZ // 2)
                part = midbuf[pair, h].astype(F32)
                squares = squares + part * part
                parts.append((part * mgain_wide[pl.ds(column, 1), :]).astype(BF16))
                columns.append(column)
        left = jnp.concatenate(parts, axis=1)
        gate = gate + jnp.dot(left, jnp.concatenate([wgt[p] for p in columns], axis=0), preferred_element_type=F32)
        upper = upper + jnp.dot(left, jnp.concatenate([wut[p] for p in columns], axis=0), preferred_element_type=F32)
    scale = lax.rsqrt(row_sum(squares) / width + 1e-5)
    gate = gate * scale
    act = (gate / (1.0 + jnp.exp(-gate)) * (upper * scale)).astype(BF16)
    scatter(4, act, wd, dsend, drecv, d_sem)
    sent(3, some(midbuf, len(MID_OFFSETS)))
    total = gathered(dsend, drecv, d_sem)
    mid_own = midbuf[mine, lax.shift_right_logical(z, 2)]
    out_ref[...] = (mid_own.astype(F32) + total).astype(BF16)
    sent(4, some(dsend, N - 1))


def per_device(*args):
    (hidden_in, attn_gain, w_query, w_key, w_value, key_cache, value_cache, write_pos, cache_len, w_out, mlp_gain,
     w_gate, w_up, w_down) = args
    seqs, width = hidden_in.shape
    lines = width // 128
    attn_gain = attn_gain.reshape(lines, 128)
    mlp_gain = mlp_gain.reshape(lines, 128)
    w_key, w_value, w_gate, w_up = w_key.T, w_value.T, w_gate.T, w_up.T
    operands = (hidden_in, attn_gain, w_query, w_key, w_value, key_cache, value_cache, write_pos, cache_len, w_out,
                mlp_gain, w_gate, w_up, w_down)
    held = [pltpu.VMEM(a.shape, a.dtype) for a in operands]
    held[7] = pltpu.SMEM(write_pos.shape, write_pos.dtype)
    held[8] = pltpu.SMEM(cache_len.shape, cache_len.dtype)
    for i in (5, 6):
        held[i] = pltpu.VMEM((KV_HEADS, *key_cache.shape[:2], HEAD_DIM), key_cache.dtype)
    for i in (9, 11, 12, 13):
        held[i] = pltpu.VMEM((lines, operands[i].shape[0], 128), operands[i].dtype)
    block = (N, seqs, 128)
    return pl.pallas_call(
        kernel,
        out_shape=pltpu.VMEM((seqs, 128), BF16),
        in_specs=[pl.BlockSpec(memory_space=pltpu.HBM)] * len(operands),
        out_specs=pl.BlockSpec(memory_space=pltpu.VMEM),
        scratch_shapes=held
        + [
            pltpu.VMEM(block, BF16),
            pltpu.VMEM((GROUP, 2, seqs, 128), BF16),
            pltpu.VMEM((N, 2, seqs, 128), BF16),
            pltpu.VMEM((N, 2, seqs, 128), BF16),
            pltpu.VMEM((N // 2, 2, seqs, 128), BF16),
            pltpu.VMEM((N, 2, seqs, 128), BF16),
            pltpu.VMEM((N // 2, 2, seqs, 128), BF16),
            pltpu.VMEM(block, BF16),
            pltpu.VMEM(block, BF16),
            pltpu.VMEM((lines, 128), F32),
            pltpu.VMEM((KV_HEADS, seqs, HEAD_DIM, key_cache.shape[1]), BF16),
            pltpu.VMEM((lines, 128, w_gate.shape[0]), BF16),
            pltpu.VMEM((lines, 128, w_up.shape[0]), BF16),
            pltpu.SemaphoreType.DMA((len(operands),)),
            pltpu.SemaphoreType.DMA((6,)),
            pltpu.SemaphoreType.DMA((1,)),
            pltpu.SemaphoreType.DMA((1,)),
            pltpu.SemaphoreType.DMA((2,)),
            pltpu.SemaphoreType.DMA((1,)),
            pltpu.SemaphoreType.DMA((len(MID_CLASSES),)),
            pltpu.SemaphoreType.DMA((2,)),
        ],
        compiler_params=pltpu.CompilerParams(
            collective_id=0, has_side_effects=True, vmem_limit_bytes=67026944
        ),
    )(*operands)


def solution(mesh):
    in_specs = (
        P("batch", None),
        P(),
        P(None, "cache"),
        P(None, "cache"),
        P(None, "cache"),
        P("batch", "cache", None),
        P("batch", "cache", None),
        P("batch"),
        P("batch"),
        P("cache", None),
        P(),
        P(None, "cache"),
        P(None, "cache"),
        P("cache", None),
    )
    return jax.shard_map(
        per_device, mesh=mesh, in_specs=in_specs, out_specs=P("batch", "cache"), check_vma=False
    )
```
